256 devices in a mesh: grp: 8 (over x, z_lo), facet: 32 (over z_hi, y, core).
Axes of the slice: x: 4, y: 4, z: 8 (z_hi: 4, z_lo: 2; z = z_hi * 2 + z_lo), core: 2. Of those that a mesh axis runs over, the one named last changes fastest.
Arguments:
- image: float32 [16, 512, 1024], P(None, 'facet', 'grp'), may hold values from 0 to 2
- wavelet_dual: bfloat16 [8, 16, 512, 1024], P(None, None, 'facet', 'grp'), may hold values from -6 to 6
- thresholds: float32 [8, 512, 1024], P(None, 'facet', 'grp'), may hold values from 1 to 10
- filter_taps: float32 [8, 2, 7], replicated, may hold values from -2 to 2
- visibilities: float32 [32, 8, 8, 16, 256], P('facet', 'grp'), may hold values from -6 to 6
- data_dual: float32 [32, 8, 8, 16, 256], P('facet', 'grp'), may hold values from -6 to 6
- ball_radii: float32 [32, 8, 8], P('facet', 'grp'), may hold values from 19.2 to 256
- blocks: bfloat16 [32, 8, 16, 256, 256], P('facet', 'grp'), may hold values from -0.375 to 0.375
- row_index: int32 [32, 8, 16], P('facet', 'grp'), may hold values from 0 to 7
- col_index: int32 [32, 8, 16], P('facet', 'grp'), may hold values from 0 to 23
Outputs:
- image_out: float32 [16, 512, 1024], P(None, 'facet', 'grp')
- data_dual_out: float32 [32, 8, 8, 16, 256], P('facet', 'grp')
- wavelet_dual_out: bfloat16 [8, 16, 512, 1024], P(None, None, 'facet', 'grp')
The draws below stay inside these ranges and needn't reach their ends.
Inputs may be any that keep to these rules, and one draw needn't show every extreme that they name: `row_index`: the visibility block of the same device that an operator block feeds. `col_index`: a tile of the band of three facets (the facet above, the device's own, the facet below) over the device's 128 columns, numbered row of tiles by row of tiles, 8 tiles a row.
All inputs are finite; a program needn't handle non-finite values.
Results may differ from the reference program's by a relative error of at most 0.0071.
Values may be sent and summed in bfloat16 or wider, within the bound.
No kernel may reach another device: no remote copies, remote signals or barrier semaphores. Data moves between devices by JAX's collectives and lax.ppermute only.
A program may use at most 64 MiB of HBM per device.

```python
import math
import jax
import jax.numpy as jnp
from jax import lax

C = 16
NB = 8
W = 3
TS = 16
ITERS = 2
RF = 16
CG = 128
VB = 256
KDEV = 16
RB = 8
FACETS = 32
GROUPS = 8
NY = 512
NX = 1024
PIX = 256
TAPS = 7
NT3 = 24


def with_ends(result, own_key, smallest, high):
    longest = result.shape.index(max(result.shape))
    spots = []
    for shift in (0, 1):
        where = [jax.random.randint(jax.random.fold_in(own_key, axis), (), 0, length) for axis, length in enumerate(result.shape)]
        where[longest] = (where[longest] + shift) % result.shape[longest]
        spots.append(tuple(where))
    return result.at[spots[0]].set(smallest).at[spots[1]].set(high)


def steps_of(own_key, dims, pieces, least, high):
    def one(position, blocks):
        heights = jax.random.uniform(jax.random.fold_in(jax.random.fold_in(own_key, 6), position), (blocks,), jnp.float32, least / len(pieces), high / len(pieces))
        return jnp.repeat(jnp.exp(heights), dims[position] // blocks).reshape((-1,) + (1,) * (len(dims) - position - 1))

    level = one(*pieces[0])
    for cut in pieces[1:]:
        level = level * one(*cut)
    return level


def noise(own_key, extent, scale, bound, pieces=(), kind=jnp.bfloat16):
    entries = jax.random.normal(own_key, extent, jnp.float32) * scale
    if len(pieces) > 0:
        entries = steps_of(own_key, extent, pieces, -0.22, 0.18) * entries
    return jnp.clip(entries, min=-bound, max=bound).astype(kind)


def setup_inputs(seed: int = 0) -> dict:
    arg_keys = jax.random.split(jax.random.key(seed), 11)
    return {
        "image": jnp.clip(2.0 * jax.random.uniform(arg_keys[0], (C, NY, NX), jnp.float32) ** steps_of(arg_keys[0], (C, NY, NX), ((1, 32), (2, 8)), -0.2, 0.2), 0.0, 2.0),
        "wavelet_dual": noise(arg_keys[1], (NB, C, NY, NX), 1.0, 6.0, ((2, 32), (3, 8))),
        "thresholds": jnp.clip(jnp.exp(math.log(10.0) - 2.3025851 * jax.random.uniform(arg_keys[2], (NB, NY, NX), jnp.float32) ** steps_of(arg_keys[2], (NB, NY, NX), ((1, 32), (2, 8)), -0.2, 0.2)), 1.0, 10.0),
        "filter_taps": noise(arg_keys[3], (NB, 2, TAPS), TAPS ** -0.5, 2.0, (), jnp.float32),
        "visibilities": noise(arg_keys[4], (FACETS, GROUPS, RB, C, VB), 1.0, 6.0, ((0, 32), (1, 8)), jnp.float32),
        "data_dual": noise(arg_keys[5], (FACETS, GROUPS, RB, C, VB), 1.0, 6.0, ((0, 32), (1, 8)), jnp.float32),
        "ball_radii": jnp.clip(jnp.exp(math.log(256.0) - 2.5902671 * jax.random.uniform(arg_keys[6], (FACETS, GROUPS, RB), jnp.float32) ** steps_of(arg_keys[6], (FACETS, GROUPS, RB), ((0, 32), (1, 8)), -0.2, 0.2)), 19.2, 256.0),
        "blocks": noise(arg_keys[7], (FACETS, GROUPS, KDEV, PIX, VB), PIX ** -0.5, 0.375, ((0, 32), (1, 8))),
        "row_index": with_ends(jax.random.randint(arg_keys[8], (FACETS, GROUPS, KDEV), 0, RB), jax.random.fold_in(arg_keys[8], 1), 0, RB - 1).astype(jnp.int32),
        "col_index": with_ends(jax.random.randint(arg_keys[9], (FACETS, GROUPS, KDEV), 0, NT3), jax.random.fold_in(arg_keys[9], 1), 0, NT3 - 1).astype(jnp.int32),
    }


step_primal = 0.5
step_data = 0.5
step_wave = 0.5

def tile_coords(col_index):
    per_row = CG // TS
    facet_ids = lax.broadcasted_iota(jnp.int32, col_index.shape, 0)
    group_ids = lax.broadcasted_iota(jnp.int32, col_index.shape, 1)
    tile_rows = facet_ids * (RF // TS) + col_index // per_row
    tile_cols = group_ids * per_row + col_index % per_row
    return (tile_rows.astype(jnp.int32), tile_cols.astype(jnp.int32))

def to_tiles(picture):
    channels, height, width = picture.shape
    shaped = picture.reshape(channels, height // TS, TS, width // TS, TS)
    return shaped.transpose(1, 3, 0, 2, 4).reshape(height // TS, width // TS, channels, TS * TS)

def from_tiles(tile_grid):
    tile_high, tile_wide, channels, pixels = tile_grid.shape
    shaped = tile_grid.reshape(tile_high, tile_wide, channels, TS, TS)
    return shaped.transpose(2, 0, 3, 1, 4).reshape(channels, tile_high * TS, tile_wide * TS)

def measure(picture, blocks, row_index, col_index):
    padded = jnp.pad(picture, ((0, 0), (RF, RF), (0, 0)))
    tile_grid = to_tiles(padded)
    tile_rows, tile_cols = tile_coords(col_index)
    picked = tile_grid[tile_rows, tile_cols]

    def one_facet(inputs):
        tile_set, operators, row_ids = inputs
        products = jnp.einsum('gkcp,gkpv->gkcv', tile_set.astype(jnp.float32), operators.astype(jnp.float32), precision=lax.Precision.HIGHEST)
        selector = (row_ids[:, :, None] == jnp.arange(RB, dtype=jnp.int32)[None, None, :]).astype(jnp.float32)
        return jnp.einsum('gkr,gkcv->grcv', selector, products, precision=lax.Precision.HIGHEST)
    return lax.map(one_facet, (picked, blocks, row_index))

def back_project(duals, blocks, row_index, col_index):
    group_ids = jnp.arange(GROUPS, dtype=jnp.int32)[:, None]

    def one_facet(inputs):
        dual_set, operators, row_ids = inputs
        picked = dual_set[group_ids, row_ids]
        return jnp.einsum('gkcv,gkpv->gkcp', picked.astype(jnp.float32), operators.astype(jnp.float32), precision=lax.Precision.HIGHEST)
    contrib = lax.map(one_facet, (duals, blocks, row_index))
    tile_rows, tile_cols = tile_coords(col_index)
    tile_grid = jnp.zeros(((NY + 2 * RF) // TS, NX // TS, C, TS * TS), jnp.float32)
    tile_grid = tile_grid.at[tile_rows, tile_cols].add(contrib)
    return from_tiles(tile_grid)[:, RF:RF + NY, :]

def analysis(picture, taps):
    height, width = (picture.shape[1], picture.shape[2])
    padded = jnp.pad(picture, ((0, 0), (W, W), (W, W)))
    row_sums = jnp.zeros((picture.shape[0], height, width + 2 * W), jnp.float32)
    for tap in range(TAPS):
        row_sums = row_sums + taps[0, tap] * padded[:, tap:tap + height, :]
    total = jnp.zeros(picture.shape, jnp.float32)
    for tap in range(TAPS):
        total = total + taps[1, tap] * row_sums[:, :, tap:tap + width]
    return total

def synthesis(duals, taps):
    height, width = (duals.shape[1], duals.shape[2])
    padded = jnp.pad(duals, ((0, 0), (W, W), (W, W)))
    row_sums = jnp.zeros((duals.shape[0], height, width + 2 * W), jnp.float32)
    for tap in range(TAPS):
        row_sums = row_sums + taps[0, tap] * padded[:, 2 * W - tap:2 * W - tap + height, :]
    total = jnp.zeros(duals.shape, jnp.float32)
    for tap in range(TAPS):
        total = total + taps[1, tap] * row_sums[:, :, 2 * W - tap:2 * W - tap + width]
    return total

def reference(image, wavelet_dual, thresholds, filter_taps, visibilities, data_dual, ball_radii, blocks, row_index, col_index):
    primal = image
    dual_data = data_dual
    dual_wave = wavelet_dual
    for iteration in range(ITERS):
        backward = back_project(dual_data.astype(jnp.bfloat16), blocks, row_index, col_index)
        smooth = jnp.zeros(primal.shape, jnp.float32)
        for basis in range(NB):
            smooth = smooth + synthesis(dual_wave[basis].astype(jnp.float32), filter_taps[basis])
        updated = jnp.maximum(primal - step_primal * (backward + smooth), 0.0)
        extrap = (2.0 * updated - primal).astype(jnp.bfloat16)
        prediction = measure(extrap, blocks, row_index, col_index)
        moved = dual_data + step_data * prediction
        offset = moved / step_data - visibilities
        length = jnp.sqrt(lax.optimization_barrier(jnp.sum(offset * offset, axis=(3, 4))))
        nearest = visibilities + offset * (ball_radii / jnp.maximum(length, ball_radii))[..., None, None]
        dual_data = moved - step_data * nearest
        extrap_wide = extrap.astype(jnp.float32)
        new_wave = []
        for basis in range(NB):
            widened = dual_wave[basis].astype(jnp.float32) + step_wave * analysis(extrap_wide, filter_taps[basis])
            magnitude = jnp.sqrt(lax.optimization_barrier(jnp.sum(widened * widened, axis=0)))
            shrink = thresholds[basis] / jnp.maximum(magnitude, thresholds[basis])
            new_wave.append((widened * shrink[None]).astype(jnp.bfloat16))
        dual_wave = jnp.stack(new_wave)
        primal = updated
    return (primal, dual_data, dual_wave)
```

```python
import jax
import jax.numpy as jnp
from jax import lax
from jax.experimental import pallas as pl
from jax.experimental.pallas import tpu as pltpu
from jax.sharding import PartitionSpec as P

ITERS = 2
NB = 8
C = 16
R = 16
L = 128
W = 3
TAPS = 7
RB = 8
KDEV = 16
NT3 = 24
VB = 256
RE = R + 2 * W
BAND = 3 * R
F32 = jnp.float32
BF16 = jnp.bfloat16

VMEM = pl.BlockSpec(memory_space=pltpu.VMEM)
SMEM = pl.BlockSpec(memory_space=pltpu.SMEM)


def lanes():
    return lax.broadcasted_iota(jnp.int32, (C, L), 1)


def roll(x, shift):
    shift = shift % L
    return x if shift == 0 else pltpu.roll(x, shift, 1)


def is_odd(axis):
    return lax.rem(lax.axis_index(axis), 2) == 1


def pack(rows):
    total = rows[0]
    for i in range(1, len(rows)):
        total = total + roll(rows[i], 8 * i)
    return total


def unpack(packed, i, lane):
    return jnp.where(lane < 6, roll(packed, -8 * i), 0.0)


def swap_blocks(xs):
    xs = list(xs)
    lane = lanes()
    for bit in range(3):
        m = 1 << bit
        low = (lane // (16 * m)) % 2 == 0
        for i in range(8):
            if i & m == 0:
                a, b = xs[i], xs[i | m]
                xs[i] = jnp.where(low, a, roll(b, 16 * m))
                xs[i | m] = jnp.where(low, roll(a, -16 * m), b)
    return xs


def build_columns(taps, high, low):
    n = lax.broadcasted_iota(jnp.int32, (L, 2 * L), 1)
    j = lax.broadcasted_iota(jnp.int32, (L, 2 * L), 0)
    place = jnp.where(n < L, n, jnp.where(n < L + W, n - L - W, n - W))
    tap = jnp.where(n < L + 2 * W, place - j + W, -1)
    for b in range(NB):
        value = jnp.zeros((L, 2 * L), F32)
        for e in range(TAPS):
            value = jnp.where(tap == e, taps[b, 1, e], value)
        rounded = value.astype(BF16)
        high[b * L : (b + 1) * L, :] = rounded
        low[b * L : (b + 1) * L, :] = (value - rounded.astype(F32)).astype(BF16)


def back_project(vb, blocks, row_ids, col_ids, contrib, sums):
    for k in range(KDEV):
        contrib[k] = lax.dot_general(
            vb[row_ids[k]], blocks[k], (((1,), (1,)), ((), ())), preferred_element_type=F32
        )
    sums[...] = jnp.zeros(sums.shape, F32)
    for k in range(KDEV):
        q = col_ids[k]
        sums[q] = sums[q] + contrib[k]


def synth_rows(taps, b, rows, wide_h, wide_l):
    for i in range(RE):
        total = None
        for a in range(TAPS):
            r = i - a
            if 0 <= r < R:
                term = taps[b, 0, a] * rows[r]
                total = term if total is None else total + term
        high = total.astype(BF16)
        wide_h[i * C : (i + 1) * C, b * L : (b + 1) * L] = high
        wide_l[i * C : (i + 1) * C, b * L : (b + 1) * L] = (total - high.astype(F32)).astype(BF16)


def finish_backward(sums, wide_h, wide_l, col_h, col_l, smooth, main, ext, msg):
    wh = wide_h[...]
    smooth[...] = (
        jnp.dot(wh, col_h[...], preferred_element_type=F32)
        + jnp.dot(wide_l[...], col_h[...], preferred_element_type=F32)
        + jnp.dot(wh, col_l[...], preferred_element_type=F32)
    )
    for tr in range(3):
        for h in range(2):
            xs = swap_blocks([sums[tr * 8 + t, :, h * L : (h + 1) * L] for t in range(8)])
            for i in range(8):
                r = tr * R + h * 8 + i
                t = r - (R - W)
                value = xs[i]
                if 0 <= t < RE:
                    value = value + smooth[t * C : (t + 1) * C, :L]
                main[r] = value
    for t in range(RE):
        ext[t] = smooth[t * C : (t + 1) * C, L:]
    odd = is_odd("facet")
    base = jnp.where(odd, 0, 2 * R)
    base_ext = jnp.where(odd, 0, R + W)
    for r in range(R):
        msg[r] = main[base + r].astype(BF16)
    msg[R] = pack([ext[base_ext + i] for i in range(W)]).astype(BF16)


def first_kernel(
    taps, row_ids, col_ids, u, v, blocks,
    main, ext, msg, u_rows, col_h, col_l,
    vb, contrib, sums, turned, wide_h, wide_l, smooth,
):
    build_columns(taps, col_h, col_l)
    vb[...] = v[...].astype(BF16)
    back_project(vb, blocks, row_ids, col_ids, contrib, sums)
    for b in range(NB):
        turned[b] = u[b].astype(F32)
        rows = [turned[b, pl.ds(r, C, stride=R), :] for r in range(R)]
        for r in range(R):
            u_rows[b, r * C : (r + 1) * C, :] = rows[r].astype(BF16)
        synth_rows(taps, b, rows, wide_h, wide_l)
    finish_backward(sums, wide_h, wide_l, col_h, col_l, smooth, main, ext, msg)


def pair_kernel(with_image, *refs):
    if with_image:
        main, ext, got, image, total, total_ext, msg = refs
    else:
        main, ext, got, total, total_ext, msg = refs
    odd = is_odd("facet")
    lane = lanes()
    for r in range(R):
        row = main[R + r] + got[r].astype(F32)
        total[r] = row
        msg[R + r] = row.astype(BF16)
        total_ext[r] = ext[W + r]
    spot = jnp.where(odd, 0, R - W)
    packed = got[R].astype(F32)
    for i in range(W):
        total_ext[spot + i] = total_ext[spot + i] + unpack(packed, i, lane)
    far = jnp.where(odd, 2 * R, 0)
    far_ext = jnp.where(odd, R + W, 0)
    for r in range(R):
        msg[r] = main[far + r].astype(BF16)
    msg[2 * R] = pack([total_ext[r] for r in range(R)]).astype(BF16)
    msg[2 * R + 1] = pack([ext[far_ext + i] for i in range(W)]).astype(BF16)
    if with_image:
        for r in range(R):
            msg[2 * R + 2 + r] = image[pl.ds(r, C, stride=R), :].astype(BF16)


def rim_kernel(with_image, *refs):
    if with_image:
        total, total_ext, main, ext, got, image, part, part_ext, msg_a, msg_b, x = refs
    else:
        total, total_ext, main, ext, got, part, part_ext, msg_a, msg_b = refs
    odd = is_odd("facet")
    lane = lanes()
    far = jnp.where(odd, 2 * R, 0)
    far_ext = jnp.where(odd, R + W, 0)
    packed = got[2 * R].astype(F32)
    for r in range(R):
        part[r] = total[r] + got[r].astype(F32)
        part_ext[r] = total_ext[r]
        part[R + r] = got[R + r].astype(F32) + main[far + r]
        part_ext[R + r] = unpack(packed, r, lane)
    near = jnp.where(odd, R - W, 0)
    away = jnp.where(odd, 0, R - W)
    packed = got[2 * R + 1].astype(F32)
    for i in range(W):
        part_ext[near + i] = part_ext[near + i] + unpack(packed, i, lane)
        part_ext[R + away + i] = part_ext[R + away + i] + ext[far_ext + i]
    if with_image:
        for r in range(R):
            x[r] = image[pl.ds(r, C, stride=R), :]
            x[R + r] = got[2 * R + 2 + r].astype(F32)
    godd = is_odd("grp")
    slot = lane // 8
    sub = lane % 8
    first = sub < W
    second = (sub >= W) & (sub < 2 * W)
    for p in range(2):
        left = jnp.zeros((C, L), F32)
        right = jnp.zeros((C, L), F32)
        for r in range(R):
            row, row_ext = part[p * R + r], part_ext[p * R + r]
            one = (slot == r) & first
            two = (slot == r) & second
            left = jnp.where(one, roll(row_ext, 8 * r), left)
            left = jnp.where(two, roll(row, 8 * r + W), left)
            right = jnp.where(one, roll(row_ext, 8 * r - W), right)
            right = jnp.where(two, roll(row, 8 * r + 2 * W), right)
        msg_a[p] = jnp.where(godd, left, right).astype(BF16)
        msg_b[p] = jnp.where(godd, right, left).astype(BF16)
        if with_image:
            left = jnp.zeros((C, L), F32)
            right = jnp.zeros((C, L), F32)
            for r in range(R):
                row = x[p * R + r]
                one = (slot == r) & first
                left = jnp.where(one, roll(row, 8 * r), left)
                right = jnp.where(one, roll(row, 8 * r + W), right)
            msg_a[2 + p] = jnp.where(godd, left, right).astype(BF16)
            msg_b[2 + p] = jnp.where(godd, right, left).astype(BF16)


def primal_kernel(first, last, *refs):
    refs = list(refs)
    part, part_ext, got_a, got_b, x = refs[:5]
    refs = refs[5:]
    if not first:
        x_ext = refs.pop(0)
    if last:
        image_out, e, e_ext, msg, turned = refs
    else:
        new_x, new_x_ext, e, e_ext, msg = refs
    lane = lanes()
    facet, grp = lax.axis_index("facet"), lax.axis_index("grp")
    odd = is_odd("facet")
    godd = is_odd("grp")
    on_left = (grp > 0) & (lane < W)
    on_right = (grp < lax.axis_size("grp") - 1) & (lane >= W) & (lane < 2 * W)
    inside = on_left | on_right
    there = jnp.where(odd, facet < lax.axis_size("facet") - 1, facet > 0)
    got_a_wide = got_a[...].astype(F32)
    got_b_wide = got_b[...].astype(F32)
    from_left = jnp.where(godd, got_a_wide, got_b_wide)
    from_right = jnp.where(godd, got_b_wide, got_a_wide)
    rims = []
    for p in range(2):
        for r in range(R):
            i = p * R + r
            grad = part[i] + jnp.where(lane < W, roll(from_left[p], -8 * r), 0.0)
            grad = grad + jnp.where(lane >= L - W, roll(from_right[p], -8 * r - W), 0.0)
            rim = jnp.where(
                lane < W, roll(from_left[p], -8 * r - W), roll(from_right[p], -8 * r)
            )
            grad_ext = part_ext[i] + rim
            old = x[i]
            if first:
                old_ext = jnp.where(
                    lane < W, roll(from_left[2 + p], -8 * r), roll(from_right[2 + p], -8 * r + W)
                )
            else:
                old_ext = x_ext[i]
            new = jnp.maximum(old - 0.5 * grad, 0.0)
            new_ext = jnp.maximum(old_ext - 0.5 * grad_ext, 0.0)
            ahead = 2.0 * new - old
            ahead_ext = jnp.where(inside, 2.0 * new_ext - old_ext, 0.0)
            if p == 1:
                ahead = jnp.where(there, ahead, 0.0)
                ahead_ext = jnp.where(there, ahead_ext, 0.0)
            e[i] = ahead.astype(BF16)
            e_ext[i] = ahead_ext.astype(BF16)
            if p == 0:
                msg[r] = ahead.astype(BF16)
                rims.append(ahead_ext)
                if last:
                    turned[r * C : (r + 1) * C, :] = new
            if not last:
                new_x[i] = new
                new_x_ext[i] = new_ext
    msg[R] = pack(rims).astype(BF16)
    if last:
        for c in range(C):
            image_out[c * R : (c + 1) * R, :] = turned[pl.ds(c, R, stride=C), :]


def dual_kernel(last, *refs):
    taps, row_ids, col_ids, radii, e, e_ext, got, v, vis, blocks, u_rows, thr, col_h, col_l = refs[:14]
    refs = refs[14:]
    if last:
        v_out, u_out, band, band_ext, near, wide, flat, contrib, sums, turned = refs
    else:
        main, ext, msg, v_out, u_out = refs[:5]
        band, band_ext, near, wide, flat, contrib, sums, turned, vb, tiles, wide_h, wide_l, smooth = refs[5:]
    odd = is_odd("facet")
    lane = lanes()
    base_a = jnp.where(odd, 0, 2 * R)
    base_b = jnp.where(odd, 2 * R, 0)
    packed = got[R].astype(F32)
    for r in range(R):
        band[R + r] = e[r].astype(F32)
        band[base_b + r] = e[R + r].astype(F32)
        band[base_a + r] = got[r].astype(F32)
        band_ext[R + r] = e_ext[r].astype(F32)
        band_ext[base_b + r] = e_ext[R + r].astype(F32)
        band_ext[base_a + r] = unpack(packed, r, lane)
    for t in range(RE):
        near[t * C : (t + 1) * C, :L] = band[R - W + t].astype(BF16)
        near[t * C : (t + 1) * C, L:] = band_ext[R - W + t].astype(BF16)
    for tr in range(3):
        for h in range(2):
            xs = swap_blocks([band[tr * R + h * 8 + i] for i in range(8)])
            for t in range(8):
                flat[tr * 8 + t, :, h * L : (h + 1) * L] = xs[t].astype(BF16)
    for k in range(KDEV):
        contrib[k] = jnp.dot(flat[col_ids[k]], blocks[k], preferred_element_type=F32)
    sums[...] = jnp.zeros(sums.shape, F32)
    for k in range(KDEV):
        r = row_ids[k]
        sums[r] = sums[r] + contrib[k]
    for r in range(RB):
        seen = vis[r]
        moved = v[r] + 0.5 * sums[r]
        offset = 2.0 * moved - seen
        length = jnp.sqrt(jnp.sum(jnp.sum(offset * offset, axis=1, keepdims=True), axis=0, keepdims=True))
        scale = radii[r] / jnp.maximum(length, radii[r])
        new = moved - 0.5 * (seen + offset * scale)
        v_out[r] = new
        if not last:
            vb[r] = new.astype(BF16)
    both = (((1,), (1,)), ((), ()))
    wide[...] = lax.dot_general(
        near[...], col_h[...], both, preferred_element_type=F32
    ) + lax.dot_general(near[...], col_l[...], both, preferred_element_type=F32)
    if not last:
        back_project(vb, blocks, row_ids, col_ids, tiles[0], tiles[1])
    for b in range(NB):
        rows = []
        for r in range(R):
            total = None
            for a in range(TAPS):
                term = taps[b, 0, a] * wide[(r + a) * C : (r + a + 1) * C, b * L : (b + 1) * L]
                total = term if total is None else total + term
            full = u_rows[b, r * C : (r + 1) * C, :].astype(F32) + 0.5 * total
            size = jnp.sqrt(jnp.sum(full * full, axis=0, keepdims=True))
            limit = thr[b, r : r + 1, :]
            new = full * (limit / jnp.maximum(size, limit))
            if last:
                turned[b, r * C : (r + 1) * C, :] = new
            else:
                new = new.astype(BF16)
                u_out[b, r * C : (r + 1) * C, :] = new
                rows.append(new.astype(F32))
        if last:
            for c in range(C):
                u_out[b, c * R : (c + 1) * R, :] = turned[b, pl.ds(c, R, stride=C), :].astype(BF16)
        else:
            synth_rows(taps, b, rows, wide_h, wide_l)
    if not last:
        finish_backward(tiles[1], wide_h, wide_l, col_h, col_l, smooth, main, ext, msg)


def shape(dims, dtype=F32):
    return jax.ShapeDtypeStruct(dims, dtype)


def scratch(*dims, dtype=F32):
    return pltpu.VMEM(dims, dtype)


BACK = [shape((BAND, C, L)), shape((RE, C, L)), shape((R + 1, C, L), BF16)]


def call(kernel, scalars, arrays, outs, temps=(), name=None):
    return pl.pallas_call(
        kernel,
        out_shape=tuple(outs),
        in_specs=[SMEM] * len(scalars) + [VMEM] * len(arrays),
        out_specs=tuple(VMEM for _ in outs),
        scratch_shapes=list(temps),
        name=name,
    )(*scalars, *arrays)


def pairs_of(axis):
    count = lax.axis_size(axis)
    inner = [(i, i ^ 1) for i in range(count)]
    outer = [(i, ((i + 1) ^ 1) - 1) for i in range(1, count - 1)]
    return inner, outer


def per_device(
    image, wavelet_dual, thresholds, filter_taps, visibilities,
    data_dual, ball_radii, blocks, row_index, col_index,
):
    image_rows = image.reshape(C * R, L)
    u = wavelet_dual.reshape(NB, C * R, L)
    operators, seen, v = blocks[0, 0], visibilities[0, 0], data_dual[0, 0]
    radii, row_ids, col_ids = ball_radii[0, 0], row_index[0, 0], col_index[0, 0]
    facet_in, facet_out = pairs_of("facet")
    grp_in, grp_out = pairs_of("grp")
    synth_temps = [
        scratch(NB, C * R, L),
        scratch(RE * C, NB * L, dtype=BF16),
        scratch(RE * C, NB * L, dtype=BF16),
        scratch(RE * C, 2 * L),
    ]
    main, ext, msg, u, col_h, col_l = call(
        first_kernel,
        (filter_taps, row_ids, col_ids),
        (u, v, operators),
        BACK
        + [shape((NB, R * C, L), BF16), shape((NB * L, 2 * L), BF16), shape((NB * L, 2 * L), BF16)],
        [scratch(RB, C, VB, dtype=BF16), scratch(KDEV, C, VB), scratch(NT3, C, VB)] + synth_temps,
        name="first",
    )
    x = x_ext = None
    for iteration in range(ITERS):
        first, last = iteration == 0, iteration == ITERS - 1
        got = lax.ppermute(msg, "facet", facet_in)
        total, total_ext, msg = call(
            lambda *refs: pair_kernel(first, *refs),
            (),
            (main, ext, got) + ((image_rows,) if first else ()),
            [
                shape((R, C, L)),
                shape((R, C, L)),
                shape(((3 if first else 2) * R + 2, C, L), BF16),
            ],
            name="pair",
        )
        got = lax.ppermute(msg, "facet", facet_out)
        rim = shape((4 if first else 2, C, L), BF16)
        part, part_ext, msg_a, msg_b, *rest = call(
            lambda *refs: rim_kernel(first, *refs),
            (),
            (total, total_ext, main, ext, got) + ((image_rows,) if first else ()),
            [shape((2 * R, C, L)), shape((2 * R, C, L)), rim, rim]
            + ([shape((2 * R, C, L))] if first else []),
            name="rim",
        )
        if first:
            x = rest[0]
        got_a = lax.ppermute(msg_a, "grp", grp_in)
        got_b = lax.ppermute(msg_b, "grp", grp_out)
        wide = shape((2 * R, C, L))
        outs = [shape((2 * R, C, L), BF16), shape((2 * R, C, L), BF16), shape((R + 1, C, L), BF16)]
        results = call(
            lambda *refs: primal_kernel(first, last, *refs),
            (),
            (part, part_ext, got_a, got_b, x) + (() if first else (x_ext,)),
            ([shape((C * R, L))] if last else [wide, wide]) + outs,
            [scratch(R * C, L)] if last else [],
            name="primal",
        )
        e, e_ext, msg = results[-3:]
        if last:
            image_out = results[0]
        else:
            x, x_ext = results[:2]
        got = lax.ppermute(msg, "facet", facet_in)
        temps = [
            scratch(BAND, C, L),
            scratch(BAND, C, L),
            scratch(RE * C, 2 * L, dtype=BF16),
            scratch(RE * C, NB * L),
            scratch(NT3, C, VB, dtype=BF16),
            scratch(KDEV, C, VB),
            scratch(RB, C, VB),
        ]
        if last:
            temps += synth_temps[:1]
        else:
            temps += [
                synth_temps[0],
                scratch(RB, C, VB, dtype=BF16),
                (scratch(KDEV, C, VB), scratch(NT3, C, VB)),
            ] + synth_temps[1:]
        *back, v, u = call(
            lambda *refs: dual_kernel(last, *refs),
            (filter_taps, row_ids, col_ids, radii),
            (e, e_ext, got, v, seen, operators, u, thresholds, col_h, col_l),
            ([] if last else BACK) + [shape((RB, C, VB)), shape((NB, R * C, L), BF16)],
            temps,
            name="dual",
        )
        if not last:
            main, ext, msg = back
    return (image_out.reshape(C, R, L), v[None, None], u.reshape(NB, C, R, L))


def solution(mesh):
    in_specs = (
        P(None, "facet", "grp"),
        P(None, None, "facet", "grp"),
        P(None, "facet", "grp"),
        P(),
        P("facet", "grp", None, None, None),
        P("facet", "grp", None, None, None),
        P("facet", "grp", None),
        P("facet", "grp", None, None, None),
        P("facet", "grp", None),
        P("facet", "grp", None),
    )
    out_specs = (
        P(None, "facet", "grp"),
        P("facet", "grp", None, None, None),
        P(None, None, "facet", "grp"),
    )
    return jax.shard_map(
        per_device, mesh=mesh, in_specs=in_specs, out_specs=out_specs, check_vma=False
    )
```

```python
import jax
import jax.numpy as jnp
from jax import lax
from jax.experimental import pallas as pl
from jax.experimental.pallas import tpu as pltpu
from jax.sharding import PartitionSpec as P

ITERS = 2
NB = 8
C = 16
R = 16
L = 128
W = 3
TAPS = 7
RB = 8
KDEV = 16
NT3 = 24
VB = 256
RE = R + 2 * W
BAND = 3 * R
F32 = jnp.float32
BF16 = jnp.bfloat16

VMEM = pl.BlockSpec(memory_space=pltpu.VMEM)


def lanes():
    return lax.broadcasted_iota(jnp.int32, (C, L), 1)


def roll(x, shift):
    shift = shift % L
    return x if shift == 0 else pltpu.roll(x, shift, 1)


def is_odd(axis):
    return lax.rem(lax.axis_index(axis), 2) == 1


def pack(rows):
    total = rows[0]
    for i in range(1, len(rows)):
        total = total + roll(rows[i], 8 * i)
    return total


def unpack(packed, i, lane):
    return jnp.where(lane < 6, roll(packed, -8 * i), 0.0)


def swap_blocks(xs):
    xs = list(xs)
    lane = lanes()
    for bit in range(3):
        m = 1 << bit
        low = (lane // (16 * m)) % 2 == 0
        for i in range(8):
            if i & m == 0:
                a, b = xs[i], xs[i | m]
                xs[i] = jnp.where(low, a, roll(b, 16 * m))
                xs[i | m] = jnp.where(low, roll(a, -16 * m), b)
    return xs


def build_columns(taps, high, low):
    n = lax.broadcasted_iota(jnp.int32, (L, 2 * L), 1)
    j = lax.broadcasted_iota(jnp.int32, (L, 2 * L), 0)
    place = jnp.where(n < L, n, jnp.where(n < L + W, n - L - W, n - W))
    tap = jnp.where(n < L + 2 * W, place - j + W, -1)
    for b in range(NB):
        value = jnp.zeros((L, 2 * L), F32)
        for e in range(TAPS):
            value = jnp.where(tap == e, taps[e, 1, b], value)
        rounded = value.astype(BF16)
        high[b * L : (b + 1) * L, :] = rounded
        low[b * L : (b + 1) * L, :] = (value - rounded.astype(F32)).astype(BF16)


def back_project(vb, blocks, row_ids, col_ids, contrib, sums):
    for k in range(KDEV):
        contrib[k] = lax.dot_general(
            vb[row_ids[k]], blocks[k], (((1,), (1,)), ((), ())), preferred_element_type=F32
        )
    sums[...] = jnp.zeros(sums.shape, F32)
    for k in range(KDEV):
        q = col_ids[k]
        sums[q] = sums[q] + contrib[k]


def synth_rows(taps, b, rows, wide_h, wide_l):
    for i in range(RE):
        total = None
        for a in range(TAPS):
            r = i - a
            if 0 <= r < R:
                term = taps[a, 0, b] * rows[r]
                total = term if total is None else total + term
        high = total.astype(BF16)
        wide_h[i * C : (i + 1) * C, b * L : (b + 1) * L] = high
        wide_l[i * C : (i + 1) * C, b * L : (b + 1) * L] = (total - high.astype(F32)).astype(BF16)


def filter_columns(rows_h, rows_l, col_h, col_l):
    return (
        jnp.dot(rows_h, col_h[...], preferred_element_type=F32)
        + jnp.dot(rows_l, col_h[...], preferred_element_type=F32)
        + jnp.dot(rows_h, col_l[...], preferred_element_type=F32)
    )


def make_message(sums, wide_h, wide_l, col_h, col_l, smooth, msg):
    odd = is_odd("facet")
    tile_row = jnp.where(odd, 0, 2)
    top = pl.multiple_of(jnp.where(odd, 0, (R + W) * C), C)
    smooth[...] = filter_columns(
        wide_h[pl.ds(top, W * C), :], wide_l[pl.ds(top, W * C), :], col_h, col_l
    )
    spot = jnp.where(odd, R - W, 0)
    for h in range(2):
        xs = swap_blocks([sums[tile_row * 8 + t, :, h * L : (h + 1) * L] for t in range(8)])
        for i in range(8):
            r = h * 8 + i
            value = xs[i]
            if r < W:
                value = value + jnp.where(odd, 0.0, smooth[r * C : (r + 1) * C, :L])
            if r >= R - W:
                t = r - (R - W)
                value = value + jnp.where(odd, smooth[t * C : (t + 1) * C, :L], 0.0)
            msg[r] = value.astype(BF16)
    msg[R] = pack([smooth[i * C : (i + 1) * C, L:] for i in range(W)]).astype(BF16)


def sums_kernel(sums, wide_h, wide_l, col_h, col_l, main, ext, smooth):
    smooth[...] = filter_columns(wide_h[...], wide_l[...], col_h, col_l)
    for tr in range(3):
        for h in range(2):
            xs = swap_blocks([sums[tr * 8 + t, :, h * L : (h + 1) * L] for t in range(8)])
            for i in range(8):
                r = tr * R + h * 8 + i
                t = r - (R - W)
                value = xs[i]
                if 0 <= t < RE:
                    value = value + smooth[t * C : (t + 1) * C, :L]
                main[r] = value
    for t in range(RE):
        ext[t] = smooth[t * C : (t + 1) * C, L:]


def fetch(sources, targets, sems):
    copies = [pltpu.make_async_copy(s, t, sems.at[i]) for i, (s, t) in enumerate(zip(sources, targets))]
    for copy in copies:
        copy.start()
    return copies


def first_kernel(
    taps_hbm, rows_hbm, cols_hbm, u_hbm, v_hbm, blocks_hbm,
    sums, wide_h, wide_l, msg, u_rows, col_h, col_l, blocks,
    taps, row_ids, col_ids, u, v, vb, contrib, turned, smooth, sems,
):
    get_taps, get_u, get_v, get_blocks, get_rows, get_cols = fetch(
        (taps_hbm, u_hbm, v_hbm, blocks_hbm, rows_hbm, cols_hbm),
        (taps, u, v, blocks, row_ids, col_ids),
        sems,
    )
    get_taps.wait()
    build_columns(taps, col_h, col_l)
    get_u.wait()
    for b in range(NB):
        turned[b] = u[b].astype(F32)
        rows = [turned[b, pl.ds(r, C, stride=R), :] for r in range(R)]
        for r in range(R):
            u_rows[b, r * C : (r + 1) * C, :] = rows[r].astype(BF16)
        synth_rows(taps, b, rows, wide_h, wide_l)
    get_v.wait()
    get_rows.wait()
    get_cols.wait()
    get_blocks.wait()
    vb[...] = v[...].astype(BF16)
    back_project(vb, blocks, row_ids, col_ids, contrib, sums)
    make_message(sums, wide_h, wide_l, col_h, col_l, smooth, msg)


def pair_kernel(with_image, *refs):
    if with_image:
        main, ext, got, image, total, total_ext, msg = refs
    else:
        main, ext, got, total, total_ext, msg = refs
    odd = is_odd("facet")
    lane = lanes()
    for r in range(R):
        row = main[R + r] + got[r].astype(F32)
        total[r] = row
        msg[R + r] = row.astype(BF16)
        total_ext[r] = ext[W + r]
    spot = jnp.where(odd, 0, R - W)
    packed = got[R].astype(F32)
    for i in range(W):
        total_ext[spot + i] = total_ext[spot + i] + unpack(packed, i, lane)
    far = jnp.where(odd, 2 * R, 0)
    far_ext = jnp.where(odd, R + W, 0)
    for r in range(R):
        msg[r] = main[far + r].astype(BF16)
    msg[2 * R] = pack([total_ext[r] for r in range(R)]).astype(BF16)
    msg[2 * R + 1] = pack([ext[far_ext + i] for i in range(W)]).astype(BF16)
    if with_image:
        for r in range(R):
            msg[2 * R + 2 + r] = image[pl.ds(r, C, stride=R), :].astype(BF16)


def rim_kernel(with_image, *refs):
    if with_image:
        total, total_ext, main, ext, got, image, part, part_ext, msg_a, msg_b, x = refs
    else:
        total, total_ext, main, ext, got, part, part_ext, msg_a, msg_b = refs
    odd = is_odd("facet")
    lane = lanes()
    far = jnp.where(odd, 2 * R, 0)
    far_ext = jnp.where(odd, R + W, 0)
    packed = got[2 * R].astype(F32)
    for r in range(R):
        part[r] = total[r] + got[r].astype(F32)
        part_ext[r] = total_ext[r]
        part[R + r] = got[R + r].astype(F32) + main[far + r]
        part_ext[R + r] = unpack(packed, r, lane)
    near = jnp.where(odd, R - W, 0)
    away = jnp.where(odd, 0, R - W)
    packed = got[2 * R + 1].astype(F32)
    for i in range(W):
        part_ext[near + i] = part_ext[near + i] + unpack(packed, i, lane)
        part_ext[R + away + i] = part_ext[R + away + i] + ext[far_ext + i]
    if with_image:
        for r in range(R):
            x[r] = image[pl.ds(r, C, stride=R), :]
            x[R + r] = got[2 * R + 2 + r].astype(F32)
    godd = is_odd("grp")
    slot = lane // 8
    sub = lane % 8
    first = sub < W
    second = (sub >= W) & (sub < 2 * W)
    for p in range(2):
        left = jnp.zeros((C, L), F32)
        right = jnp.zeros((C, L), F32)
        for r in range(R):
            row, row_ext = part[p * R + r], part_ext[p * R + r]
            one = (slot == r) & first
            two = (slot == r) & second
            left = jnp.where(one, roll(row_ext, 8 * r), left)
            left = jnp.where(two, roll(row, 8 * r + W), left)
            right = jnp.where(one, roll(row_ext, 8 * r - W), right)
            right = jnp.where(two, roll(row, 8 * r + 2 * W), right)
        msg_a[p] = jnp.where(godd, left, right).astype(BF16)
        msg_b[p] = jnp.where(godd, right, left).astype(BF16)
        if with_image:
            left = jnp.zeros((C, L), F32)
            right = jnp.zeros((C, L), F32)
            for r in range(R):
                row = x[p * R + r]
                one = (slot == r) & first
                left = jnp.where(one, roll(row, 8 * r), left)
                right = jnp.where(one, roll(row, 8 * r + W), right)
            msg_a[2 + p] = jnp.where(godd, left, right).astype(BF16)
            msg_b[2 + p] = jnp.where(godd, right, left).astype(BF16)


def primal_kernel(first, last, *refs):
    refs = list(refs)
    part, part_ext, got_a, got_b, x = refs[:5]
    refs = refs[5:]
    if not first:
        x_ext = refs.pop(0)
    if last:
        image_out, e, e_ext, msg, turned = refs
    else:
        new_x, new_x_ext, e, e_ext, msg = refs
    lane = lanes()
    facet, grp = lax.axis_index("facet"), lax.axis_index("grp")
    odd = is_odd("facet")
    godd = is_odd("grp")
    on_left = (grp > 0) & (lane < W)
    on_right = (grp < lax.axis_size("grp") - 1) & (lane >= W) & (lane < 2 * W)
    inside = on_left | on_right
    there = jnp.where(odd, facet < lax.axis_size("facet") - 1, facet > 0)
    got_a_wide = got_a[...].astype(F32)
    got_b_wide = got_b[...].astype(F32)
    from_left = jnp.where(godd, got_a_wide, got_b_wide)
    from_right = jnp.where(godd, got_b_wide, got_a_wide)
    rims = []
    for p in range(2):
        for r in range(R):
            i = p * R + r
            grad = part[i] + jnp.where(lane < W, roll(from_left[p], -8 * r), 0.0)
            grad = grad + jnp.where(lane >= L - W, roll(from_right[p], -8 * r - W), 0.0)
            rim = jnp.where(
                lane < W, roll(from_left[p], -8 * r - W), roll(from_right[p], -8 * r)
            )
            grad_ext = part_ext[i] + rim
            old = x[i]
            if first:
                old_ext = jnp.where(
                    lane < W, roll(from_left[2 + p], -8 * r), roll(from_right[2 + p], -8 * r + W)
                )
            else:
                old_ext = x_ext[i]
            new = jnp.maximum(old - 0.5 * grad, 0.0)
            new_ext = jnp.maximum(old_ext - 0.5 * grad_ext, 0.0)
            ahead = 2.0 * new - old
            ahead_ext = jnp.where(inside, 2.0 * new_ext - old_ext, 0.0)
            if p == 1:
                ahead = jnp.where(there, ahead, 0.0)
                ahead_ext = jnp.where(there, ahead_ext, 0.0)
            e[i] = ahead.astype(BF16)
            e_ext[i] = ahead_ext.astype(BF16)
            if p == 0:
                msg[r] = ahead.astype(BF16)
                rims.append(ahead_ext)
                if last:
                    turned[r * C : (r + 1) * C, :] = new
            if not last:
                new_x[i] = new
                new_x_ext[i] = new_ext
    msg[R] = pack(rims).astype(BF16)
    if last:
        for c in range(C):
            image_out[c * R : (c + 1) * R, :] = turned[pl.ds(c, R, stride=C), :]


def near_kernel(e, e_ext, col_h, col_l, flat, wide, edge):
    odd = is_odd("facet")
    base_b = jnp.where(odd, 2, 0)
    for tile_row, base in ((1, 0), (base_b, R)):
        for h in range(2):
            xs = swap_blocks([e[base + h * 8 + i].astype(F32) for i in range(8)])
            for t in range(8):
                flat[tile_row * 8 + t, :, h * L : (h + 1) * L] = xs[t].astype(BF16)
    near = jnp.concatenate([e[:R].reshape(R * C, L), e_ext[:R].reshape(R * C, L)], axis=1)
    wide[...] = spread_columns(near, col_h, col_l)
    start = jnp.where(odd, R, 2 * R - W)
    for i in range(W):
        edge[i * C : (i + 1) * C, :L] = e[start + i]
        edge[i * C : (i + 1) * C, L:] = e_ext[start + i]


def spread_columns(rows, col_h, col_l):
    both = (((1,), (1,)), ((), ()))
    return lax.dot_general(rows, col_h[...], both, preferred_element_type=F32) + lax.dot_general(
        rows, col_l[...], both, preferred_element_type=F32
    )


def dual_kernel(last, *refs):
    taps_hbm, rows_hbm, cols_hbm, radii_hbm = refs[:4]
    flat_in, inner, edge, got, v, vis, blocks, u_rows, thr, col_h, col_l = refs[4:15]
    refs = refs[15:]
    if last:
        v_hbm, u_hbm, *refs = refs
        v_out, u_out, turned, out_sems, *refs = refs
    else:
        sums, wide_h, wide_l, msg, v_out, u_out, *refs = refs
        vb, tiles, smooth, *refs = refs
    taps, row_ids, col_ids, radii, sems, flat, wide, edges, contrib, totals = refs
    get_rows, get_cols, get_radii, get_taps = fetch(
        (rows_hbm, cols_hbm, radii_hbm, taps_hbm), (row_ids, col_ids, radii, taps), sems
    )
    odd = is_odd("facet")
    lane = lanes()
    tile_a = jnp.where(odd, 0, 2)
    tile_b = jnp.where(odd, 2, 0)
    for h in range(2):
        xs = swap_blocks([got[h * 8 + i].astype(F32) for i in range(8)])
        for t in range(8):
            flat[tile_a * 8 + t, :, h * L : (h + 1) * L] = xs[t].astype(BF16)
    for t in range(8):
        flat[8 + t] = flat_in[8 + t]
        flat[tile_b * 8 + t] = flat_in[tile_b * 8 + t]
    get_rows.wait()
    get_cols.wait()
    for k in range(KDEV):
        contrib[k] = jnp.dot(flat[col_ids[k]], blocks[k], preferred_element_type=F32)
    totals[...] = jnp.zeros(totals.shape, F32)
    for k in range(KDEV):
        r = row_ids[k]
        totals[r] = totals[r] + contrib[k]
    get_radii.wait()
    for r in range(RB):
        seen = vis[r]
        moved = v[r] + 0.5 * totals[r]
        offset = 2.0 * moved - seen
        length = jnp.sqrt(jnp.sum(jnp.sum(offset * offset, axis=1, keepdims=True), axis=0, keepdims=True))
        scale = radii[r] / jnp.maximum(length, radii[r])
        new = moved - 0.5 * (seen + offset * scale)
        v_out[r] = new
        if not last:
            vb[r] = new.astype(BF16)
    if last:
        put_v = pltpu.make_async_copy(v_out, v_hbm, out_sems.at[NB])
        put_v.start()
    packed = got[R].astype(F32)
    near_a = jnp.where(odd, R - W, 0)
    above, below = edges.at[0], edges.at[1]
    for i in range(W):
        rows = slice(i * C, (i + 1) * C)
        mine = edge[rows, :]
        theirs = jnp.concatenate(
            [got[near_a + i].astype(F32), jnp.where(lane < 2 * W, jnp.where(odd, roll(packed, -8 * (R - W + i)), roll(packed, -8 * i)), 0.0)],
            axis=1,
        ).astype(BF16)
        above[rows, :] = jnp.where(odd, theirs, mine)
        below[rows, :] = jnp.where(odd, mine, theirs)
    wide[: W * C, :] = spread_columns(above[...], col_h, col_l)
    wide[W * C :, :] = spread_columns(below[...], col_h, col_l)
    if not last:
        back_project(vb, blocks, row_ids, col_ids, tiles, sums)
    get_taps.wait()

    def filtered(t, b):
        cols = slice(b * L, (b + 1) * L)
        if t < W:
            return wide[t * C : (t + 1) * C, cols]
        if t < W + R:
            return inner[(t - W) * C : (t - W + 1) * C, cols]
        return wide[(t - R) * C : (t - R + 1) * C, cols]

    puts = []
    for b in range(NB):
        rows = []
        for r in range(R):
            total = None
            for a in range(TAPS):
                term = taps[a, 0, b] * filtered(r + a, b)
                total = term if total is None else total + term
            full = u_rows[b, r * C : (r + 1) * C, :].astype(F32) + 0.5 * total
            size = jnp.sqrt(jnp.sum(full * full, axis=0, keepdims=True))
            limit = thr[b, r : r + 1, :]
            new = full * (limit / jnp.maximum(size, limit))
            if last:
                turned[b, r * C : (r + 1) * C, :] = new
            else:
                new = new.astype(BF16)
                u_out[b, r * C : (r + 1) * C, :] = new
                rows.append(new.astype(F32))
        if last:
            for c in range(C):
                u_out[b, c * R : (c + 1) * R, :] = turned[b, pl.ds(c, R, stride=C), :].astype(BF16)
            put = pltpu.make_async_copy(u_out.at[b], u_hbm.at[b], out_sems.at[b])
            put.start()
            puts.append(put)
        else:
            synth_rows(taps, b, rows, wide_h, wide_l)
    if last:
        put_v.wait()
        for put in puts:
            put.wait()
    else:
        make_message(sums, wide_h, wide_l, col_h, col_l, smooth, msg)


def shape(dims, dtype=F32):
    return jax.ShapeDtypeStruct(dims, dtype)


def scratch(*dims, dtype=F32):
    return pltpu.VMEM(dims, dtype)


def small(dims, dtype):
    return pltpu.SMEM(dims, dtype)


HALF = [shape((NT3, C, VB)), shape((RE * C, NB * L), BF16), shape((RE * C, NB * L), BF16), shape((R + 1, C, L), BF16)]


def call(kernel, far, arrays, outs, temps=(), name=None, mib=8, final=0):
    far = [pltpu.with_memory_space_constraint(a, pltpu.HBM) for a in far]
    arrays = [pltpu.with_memory_space_constraint(a, pltpu.VMEM) for a in arrays]
    anywhere = pl.BlockSpec(memory_space=pl.ANY)
    return pl.pallas_call(
        kernel,
        out_shape=tuple(
            (pltpu.HBM if i < final else pltpu.VMEM)(o.shape, o.dtype) for i, o in enumerate(outs)
        ),
        in_specs=[anywhere] * len(far) + [VMEM] * len(arrays),
        out_specs=tuple(anywhere if i < final else VMEM for i in range(len(outs))),
        scratch_shapes=list(temps),
        compiler_params=pltpu.CompilerParams(vmem_limit_bytes=mib << 20),
        name=name,
    )(*far, *arrays)


def pairs_of(axis):
    count = lax.axis_size(axis)
    inner = [(i, i ^ 1) for i in range(count)]
    outer = [(i, ((i + 1) ^ 1) - 1) for i in range(1, count - 1)]
    return inner, outer


def per_device(
    image, wavelet_dual, thresholds, filter_taps, visibilities,
    data_dual, ball_radii, blocks, row_index, col_index,
):
    image_rows = image.reshape(C * R, L)
    u = wavelet_dual.reshape(NB, C * R, L)
    seen, v = visibilities[0, 0], data_dual[0, 0]
    radii, row_ids, col_ids = ball_radii[0, 0], row_index[0, 0], col_index[0, 0]
    taps = filter_taps.transpose(2, 1, 0)
    facet_in, facet_out = pairs_of("facet")
    grp_in, grp_out = pairs_of("grp")
    scalars = [small((TAPS, 2, NB), F32), small((KDEV,), jnp.int32), small((KDEV,), jnp.int32)]
    sums, wide_h, wide_l, msg, u, col_h, col_l, operators = call(
        first_kernel,
        (taps, row_ids, col_ids, u, v, blocks[0, 0]),
        (),
        HALF
        + [
            shape((NB, R * C, L), BF16),
            shape((NB * L, 2 * L), BF16),
            shape((NB * L, 2 * L), BF16),
            shape((KDEV, VB, VB), BF16),
        ],
        scalars
        + [
            scratch(NB, C * R, L, dtype=BF16),
            scratch(RB, C, VB),
            scratch(RB, C, VB, dtype=BF16),
            scratch(KDEV, C, VB),
            scratch(NB, C * R, L),
            scratch(W * C, 2 * L),
            pltpu.SemaphoreType.DMA((6,)),
        ],
        name="first",
        mib=16,
    )
    x = x_ext = None
    for iteration in range(ITERS):
        first, last = iteration == 0, iteration == ITERS - 1
        got = lax.ppermute(msg, "facet", facet_in)
        main, ext = call(
            sums_kernel,
            (),
            (sums, wide_h, wide_l, col_h, col_l),
            [shape((BAND, C, L)), shape((RE, C, L))],
            [scratch(RE * C, 2 * L)],
            name="sums",
        )
        total, total_ext, msg = call(
            lambda *refs: pair_kernel(first, *refs),
            (),
            (main, ext, got) + ((image_rows,) if first else ()),
            [
                shape((R, C, L)),
                shape((R, C, L)),
                shape(((3 if first else 2) * R + 2, C, L), BF16),
            ],
            name="pair",
        )
        got = lax.ppermute(msg, "facet", facet_out)
        rim = shape((4 if first else 2, C, L), BF16)
        part, part_ext, msg_a, msg_b, *rest = call(
            lambda *refs: rim_kernel(first, *refs),
            (),
            (total, total_ext, main, ext, got) + ((image_rows,) if first else ()),
            [shape((2 * R, C, L)), shape((2 * R, C, L)), rim, rim]
            + ([shape((2 * R, C, L))] if first else []),
            name="rim",
        )
        if first:
            x = rest[0]
        got_a = lax.ppermute(msg_a, "grp", grp_in)
        got_b = lax.ppermute(msg_b, "grp", grp_out)
        wide = shape((2 * R, C, L))
        outs = [shape((2 * R, C, L), BF16), shape((2 * R, C, L), BF16), shape((R + 1, C, L), BF16)]
        results = call(
            lambda *refs: primal_kernel(first, last, *refs),
            (),
            (part, part_ext, got_a, got_b, x) + (() if first else (x_ext,)),
            ([shape((C * R, L))] if last else [wide, wide]) + outs,
            [scratch(R * C, L)] if last else [],
            name="primal",
        )
        e, e_ext, msg = results[-3:]
        if last:
            image_out = results[0]
        else:
            x, x_ext = results[:2]
        got = lax.ppermute(msg, "facet", facet_in)
        flat, inner, edge = call(
            near_kernel,
            (),
            (e, e_ext, col_h, col_l),
            [shape((NT3, C, VB), BF16), shape((R * C, NB * L)), shape((W * C, 2 * L), BF16)],
            name="near",
        )
        outs = [shape((RB, C, VB)), shape((NB, R * C, L), BF16)]
        if last:
            temps = [
                scratch(RB, C, VB),
                scratch(NB, C * R, L, dtype=BF16),
                scratch(NB, R * C, L),
                pltpu.SemaphoreType.DMA((NB + 1,)),
            ]
        else:
            temps = [scratch(RB, C, VB, dtype=BF16), scratch(KDEV, C, VB), scratch(W * C, 2 * L)]
        *half, v, u = call(
            lambda *refs: dual_kernel(last, *refs),
            (taps, row_ids, col_ids, radii),
            (flat, inner, edge, got, v, seen, operators, u, thresholds, col_h, col_l),
            ([] if last else HALF) + outs,
            temps
            + scalars
            + [
                small((RB,), F32),
                pltpu.SemaphoreType.DMA((4,)),
                scratch(NT3, C, VB, dtype=BF16),
                scratch(2 * W * C, NB * L),
                scratch(2, W * C, 2 * L, dtype=BF16),
                scratch(KDEV, C, VB),
                scratch(RB, C, VB),
            ],
            name="dual",
            mib=16,
            final=2 if last else 0,
        )
        if not last:
            sums, wide_h, wide_l, msg = half
    return (image_out.reshape(C, R, L), v[None, None], u.reshape(NB, C, R, L))


def solution(mesh):
    in_specs = (
        P(None, "facet", "grp"),
        P(None, None, "facet", "grp"),
        P(None, "facet", "grp"),
        P(),
        P("facet", "grp", None, None, None),
        P("facet", "grp", None, None, None),
        P("facet", "grp", None),
        P("facet", "grp", None, None, None),
        P("facet", "grp", None),
        P("facet", "grp", None),
    )
    out_specs = (
        P(None, "facet", "grp"),
        P("facet", "grp", None, None, None),
        P(None, None, "facet", "grp"),
    )
    return jax.shard_map(
        per_device, mesh=mesh, in_specs=in_specs, out_specs=out_specs, check_vma=False
    )
```

```python
import jax
import jax.numpy as jnp
from jax import lax
from jax.experimental import pallas as pl
from jax.experimental.pallas import tpu as pltpu
from jax.sharding import PartitionSpec as P

ITERS = 2
NB = 8
C = 16
R = 16
L = 128
W = 3
TAPS = 7
RB = 8
KDEV = 16
NT3 = 24
VB = 256
RE = R + 2 * W
BAND = 3 * R
F32 = jnp.float32
BF16 = jnp.bfloat16

VMEM = pl.BlockSpec(memory_space=pltpu.VMEM)


def lanes():
    return lax.broadcasted_iota(jnp.int32, (C, L), 1)


def roll(x, shift):
    shift = shift % L
    return x if shift == 0 else pltpu.roll(x, shift, 1)


def is_odd(axis):
    return lax.rem(lax.axis_index(axis), 2) == 1


def pack(rows):
    total = rows[0]
    for i in range(1, len(rows)):
        total = total + roll(rows[i], 8 * i)
    return total


def unpack(packed, i, lane):
    return jnp.where(lane < 6, roll(packed, -8 * i), 0.0)


def swap_blocks(xs):
    xs = list(xs)
    lane = lanes()
    for bit in range(3):
        m = 1 << bit
        low = (lane // (16 * m)) % 2 == 0
        for i in range(8):
            if i & m == 0:
                a, b = xs[i], xs[i | m]
                xs[i] = jnp.where(low, a, roll(b, 16 * m))
                xs[i | m] = jnp.where(low, roll(a, -16 * m), b)
    return xs


def build_columns(col_taps, high, low):
    strip = 8
    for start in range(0, L, strip):
        j = start + lax.broadcasted_iota(jnp.int32, (strip, L), 0)
        n = lax.broadcasted_iota(jnp.int32, (strip, L), 1)
        outside = jnp.where(n < W, n - W, jnp.where(n < 2 * W, n - W + L, 2 * L))
        edge = start == 0 or start == L - strip
        for tile, place in ((0, n), (1, outside)):
            tap = place - j + W
            for b in range(NB):
                value = jnp.zeros((strip, L), F32)
                if tile == 0 or edge:
                    for e in range(TAPS):
                        value = jnp.where(tap == e, col_taps[e, b], value)
                rounded = value.astype(BF16)
                rows, cols = slice(b * L + start, b * L + start + strip), slice(tile * L, (tile + 1) * L)
                high[rows, cols] = rounded
                low[rows, cols] = (value - rounded.astype(F32)).astype(BF16)


def times(tap, row):
    return (tap[None] * row.reshape(2, C // 2, L)).reshape(C, L)


def filter_row(row_taps, b, terms):
    total = None
    for a, row in terms:
        term = times(row_taps[a, b], row)
        total = term if total is None else total + term
    return total


def back_project(vb, blocks, across, row_ids, col_ids, contrib, sums):
    sums[...] = jnp.zeros(sums.shape, F32)
    for k in range(KDEV):
        contrib[k] = lax.dot_general(
            vb[row_ids[k]], blocks[k], (((1,), (int(across),)), ((), ())), preferred_element_type=F32
        )
    for k in range(KDEV):
        q = col_ids[k]
        sums[q] = sums[q] + contrib[k]


def turn_kernel(blocks, after, turned):
    for k in range(KDEV):
        turned[k] = blocks[k].T


def synth_rows(row_taps, b, rows, wide):
    for i in range(RE):
        terms = [(a, rows[i - a]) for a in range(TAPS) if 0 <= i - a < R]
        total = filter_row(row_taps, b, terms)
        wide[i * C : (i + 1) * C, b * L : (b + 1) * L] = total.astype(BF16)


def filter_columns(rows, col_h, col_l):
    return jnp.dot(rows, col_h[...], preferred_element_type=F32) + jnp.dot(
        rows, col_l[...], preferred_element_type=F32
    )


def make_message(sums, wide, col_h, col_l, smooth, msg):
    odd = is_odd("facet")
    tile_row = jnp.where(odd, 0, 2)
    top = pl.multiple_of(jnp.where(odd, 0, (R + W) * C), C)
    smooth[...] = filter_columns(wide[pl.ds(top, W * C), :], col_h, col_l)
    for h in range(2):
        xs = swap_blocks([sums[tile_row * 8 + t, :, h * L : (h + 1) * L] for t in range(8)])
        for i in range(8):
            r = h * 8 + i
            value = xs[i]
            if r < W:
                value = value + jnp.where(odd, 0.0, smooth[r * C : (r + 1) * C, :L])
            if r >= R - W:
                t = r - (R - W)
                value = value + jnp.where(odd, smooth[t * C : (t + 1) * C, :L], 0.0)
            msg[r] = value.astype(BF16)
    msg[R] = pack([smooth[i * C : (i + 1) * C, L:] for i in range(W)]).astype(BF16)


def sums_kernel(sums, wide, col_h, col_l, main, ext, smooth):
    smooth[...] = filter_columns(wide[...], col_h, col_l)
    for tr in range(3):
        for h in range(2):
            xs = swap_blocks([sums[tr * 8 + t, :, h * L : (h + 1) * L] for t in range(8)])
            for i in range(8):
                r = tr * R + h * 8 + i
                t = r - (R - W)
                value = xs[i]
                if 0 <= t < RE:
                    value = value + smooth[t * C : (t + 1) * C, :L]
                main[r] = value
    for t in range(RE):
        ext[t] = smooth[t * C : (t + 1) * C, L:]


def fetch(sources, targets, sems):
    copies = [pltpu.make_async_copy(s, t, sems.at[i]) for i, (s, t) in enumerate(zip(sources, targets))]
    for copy in copies:
        copy.start()
    return copies


def first_kernel(
    taps_hbm, rows_hbm, cols_hbm, u_hbm, v_hbm, blocks_hbm,
    sums, wide, msg, u_rows, col_h, col_l, blocks, row_taps,
    row_ids, col_ids, taps, col_taps, u, v, vb, contrib, turned, smooth, sems,
):
    get_u, get_taps, get_v, get_blocks, get_rows, get_cols = fetch(
        (u_hbm, taps_hbm, v_hbm, blocks_hbm, rows_hbm, cols_hbm),
        (u, taps, v, blocks, row_ids, col_ids),
        sems,
    )
    get_taps.wait()
    for a in range(TAPS):
        for b in range(NB):
            row_taps[a, b] = jnp.broadcast_to(taps[a, 0:1, b : b + 1], (C // 2, L))
            col_taps[a, b] = jnp.broadcast_to(taps[a, 1:2, b : b + 1], (C // 2, L))
    get_u.wait()
    for b in range(NB):
        turned[b] = u[b].astype(F32)
    build_columns(col_taps, col_h, col_l)

    def wavelets(b):
        rows = [turned[b, pl.ds(r, C, stride=R), :] for r in range(R)]
        for r in range(R):
            u_rows[b, r * C : (r + 1) * C, :] = rows[r].astype(BF16)
        synth_rows(row_taps, b, rows, wide)

    for b in range(NB):
        wavelets(b)
    get_v.wait()
    get_rows.wait()
    get_cols.wait()
    get_blocks.wait()
    vb[...] = v[...].astype(BF16)
    back_project(vb, blocks, True, row_ids, col_ids, contrib, sums)
    make_message(sums, wide, col_h, col_l, smooth, msg)


def pair_kernel(with_image, *refs):
    if with_image:
        main, ext, got, image, total, total_ext, msg = refs
    else:
        main, ext, got, total, total_ext, msg = refs
    odd = is_odd("facet")
    lane = lanes()
    for r in range(R):
        row = main[R + r] + got[r].astype(F32)
        total[r] = row
        msg[R + r] = row.astype(BF16)
        total_ext[r] = ext[W + r]
    spot = jnp.where(odd, 0, R - W)
    packed = got[R].astype(F32)
    for i in range(W):
        total_ext[spot + i] = total_ext[spot + i] + unpack(packed, i, lane)
    far = jnp.where(odd, 2 * R, 0)
    far_ext = jnp.where(odd, R + W, 0)
    for r in range(R):
        msg[r] = main[far + r].astype(BF16)
    msg[2 * R] = pack([total_ext[r] for r in range(R)]).astype(BF16)
    msg[2 * R + 1] = pack([ext[far_ext + i] for i in range(W)]).astype(BF16)
    if with_image:
        for r in range(R):
            msg[2 * R + 2 + r] = image[pl.ds(r, C, stride=R), :].astype(BF16)


def rim_kernel(with_image, *refs):
    if with_image:
        total, total_ext, main, ext, got, image, _, part, part_ext, msg_a, msg_b, x = refs
    else:
        total, total_ext, main, ext, got, part, part_ext, msg_a, msg_b = refs
    odd = is_odd("facet")
    lane = lanes()
    far = jnp.where(odd, 2 * R, 0)
    far_ext = jnp.where(odd, R + W, 0)
    packed = got[2 * R].astype(F32)
    for r in range(R):
        part[r] = total[r] + got[r].astype(F32)
        part_ext[r] = total_ext[r]
        part[R + r] = got[R + r].astype(F32) + main[far + r]
        part_ext[R + r] = unpack(packed, r, lane)
    near = jnp.where(odd, R - W, 0)
    away = jnp.where(odd, 0, R - W)
    packed = got[2 * R + 1].astype(F32)
    for i in range(W):
        part_ext[near + i] = part_ext[near + i] + unpack(packed, i, lane)
        part_ext[R + away + i] = part_ext[R + away + i] + ext[far_ext + i]
    if with_image:
        for r in range(R):
            x[r] = image[pl.ds(r, C, stride=R), :]
            x[R + r] = got[2 * R + 2 + r].astype(F32)
    godd = is_odd("grp")
    slot = lane // 8
    sub = lane % 8
    first = sub < W
    second = (sub >= W) & (sub < 2 * W)
    for p in range(2):
        left = jnp.zeros((C, L), F32)
        right = jnp.zeros((C, L), F32)
        for r in range(R):
            row, row_ext = part[p * R + r], part_ext[p * R + r]
            one = (slot == r) & first
            two = (slot == r) & second
            left = jnp.where(one, roll(row_ext, 8 * r), left)
            left = jnp.where(two, roll(row, 8 * r + W), left)
            right = jnp.where(one, roll(row_ext, 8 * r - W), right)
            right = jnp.where(two, roll(row, 8 * r + 2 * W), right)
        msg_a[p] = jnp.where(godd, left, right).astype(BF16)
        msg_b[p] = jnp.where(godd, right, left).astype(BF16)
        if with_image:
            left = jnp.zeros((C, L), F32)
            right = jnp.zeros((C, L), F32)
            for r in range(R):
                row = x[p * R + r]
                one = (slot == r) & first
                left = jnp.where(one, roll(row, 8 * r), left)
                right = jnp.where(one, roll(row, 8 * r + W), right)
            msg_a[2 + p] = jnp.where(godd, left, right).astype(BF16)
            msg_b[2 + p] = jnp.where(godd, right, left).astype(BF16)


def primal_kernel(first, last, *refs):
    refs = list(refs)
    part, part_ext, got_a, got_b, x = refs[:5]
    refs = refs[5:]
    if not first:
        x_ext = refs.pop(0)
    if last:
        image_out, e, e_ext, msg, turned = refs
    else:
        new_x, new_x_ext, e, e_ext, msg = refs
    lane = lanes()
    facet, grp = lax.axis_index("facet"), lax.axis_index("grp")
    odd = is_odd("facet")
    godd = is_odd("grp")
    on_left = (grp > 0) & (lane < W)
    on_right = (grp < lax.axis_size("grp") - 1) & (lane >= W) & (lane < 2 * W)
    inside = on_left | on_right
    there = jnp.where(odd, facet < lax.axis_size("facet") - 1, facet > 0)
    got_a_wide = got_a[...].astype(F32)
    got_b_wide = got_b[...].astype(F32)
    from_left = jnp.where(godd, got_a_wide, got_b_wide)
    from_right = jnp.where(godd, got_b_wide, got_a_wide)
    rims = []
    for p in range(2):
        for r in range(R):
            i = p * R + r
            grad = part[i] + jnp.where(lane < W, roll(from_left[p], -8 * r), 0.0)
            grad = grad + jnp.where(lane >= L - W, roll(from_right[p], -8 * r - W), 0.0)
            rim = jnp.where(
                lane < W, roll(from_left[p], -8 * r - W), roll(from_right[p], -8 * r)
            )
            grad_ext = part_ext[i] + rim
            old = x[i]
            if first:
                old_ext = jnp.where(
                    lane < W, roll(from_left[2 + p], -8 * r), roll(from_right[2 + p], -8 * r + W)
                )
            else:
                old_ext = x_ext[i]
            new = jnp.maximum(old - 0.5 * grad, 0.0)
            new_ext = jnp.maximum(old_ext - 0.5 * grad_ext, 0.0)
            ahead = 2.0 * new - old
            ahead_ext = jnp.where(inside, 2.0 * new_ext - old_ext, 0.0)
            if p == 1:
                ahead = jnp.where(there, ahead, 0.0)
                ahead_ext = jnp.where(there, ahead_ext, 0.0)
            e[i] = ahead.astype(BF16)
            e_ext[i] = ahead_ext.astype(BF16)
            if p == 0:
                msg[r] = ahead.astype(BF16)
                rims.append(ahead_ext)
                if last:
                    turned[r * C : (r + 1) * C, :] = new
            if not last:
                new_x[i] = new
                new_x_ext[i] = new_ext
    msg[R] = pack(rims).astype(BF16)
    if last:
        for c in range(C):
            image_out[c * R : (c + 1) * R, :] = turned[pl.ds(c, R, stride=C), :]


def near_kernel(e, e_ext, col_h, col_l, row_taps, flat, wide, edge, middle):
    odd = is_odd("facet")
    base_b = jnp.where(odd, 2, 0)
    for tile_row, base in ((1, 0), (base_b, R)):
        for h in range(2):
            xs = swap_blocks([e[base + h * 8 + i].astype(F32) for i in range(8)])
            for t in range(8):
                flat[tile_row * 8 + t, :, h * L : (h + 1) * L] = xs[t].astype(BF16)
    near = jnp.concatenate([e[:R].reshape(R * C, L), e_ext[:R].reshape(R * C, L)], axis=1)
    wide[...] = spread_columns(near, col_h, col_l)
    start = jnp.where(odd, R, 2 * R - W)
    for i in range(W):
        edge[i * C : (i + 1) * C, :L] = e[start + i]
        edge[i * C : (i + 1) * C, L:] = e_ext[start + i]
    for b in range(NB):
        cols = slice(b * L, (b + 1) * L)
        for r in range(W, R - W):
            terms = [(a, wide[(r - W + a) * C : (r - W + a + 1) * C, cols]) for a in range(TAPS)]
            middle[b, (r - W) * C : (r - W + 1) * C, :] = filter_row(row_taps, b, terms)


def spread_columns(rows, col_h, col_l):
    both = (((1,), (1,)), ((), ()))
    return lax.dot_general(rows, col_h[...], both, preferred_element_type=F32) + lax.dot_general(
        rows, col_l[...], both, preferred_element_type=F32
    )


def dual_kernel(last, *refs):
    flat_in, inner, edge, middle, got, v, vis, blocks, u_rows, thr, col_h, col_l = refs[:12]
    row_taps, radii, rows_vmem, cols_vmem = refs[12:16]
    refs = refs[16:]
    if last:
        image, image_hbm, v_hbm, u_hbm, *refs = refs
        v_out, u_out, turned, out_sems, *refs = refs
    else:
        blocks_turned, sums, wide_next, msg, v_out, u_out, *refs = refs
        vb, tiles, smooth, *refs = refs
    row_ids, col_ids, sems, flat, wide, edges, contrib, totals = refs
    get_rows, get_cols = fetch((rows_vmem, cols_vmem), (row_ids, col_ids), sems)
    puts = []
    if last:
        put = pltpu.make_async_copy(image, image_hbm, out_sems.at[NB + 1])
        put.start()
        puts.append(put)
    odd = is_odd("facet")
    lane = lanes()
    packed = got[R].astype(F32)
    near_a = jnp.where(odd, R - W, 0)
    above, below = edges.at[0], edges.at[1]
    for i in range(W):
        rows = slice(i * C, (i + 1) * C)
        mine = edge[rows, :]
        rim = jnp.where(odd, roll(packed, -8 * (R - W + i)), roll(packed, -8 * i))
        theirs = jnp.concatenate(
            [got[near_a + i], jnp.where(lane < 2 * W, rim, 0.0).astype(BF16)], axis=1
        )
        above[rows, :] = jnp.where(odd, theirs, mine)
        below[rows, :] = jnp.where(odd, mine, theirs)
    wide[: W * C, :] = spread_columns(above[...], col_h, col_l)
    wide[W * C :, :] = spread_columns(below[...], col_h, col_l)
    tile_a = jnp.where(odd, 0, 2)
    tile_b = jnp.where(odd, 2, 0)
    for h in range(2):
        xs = swap_blocks([got[h * 8 + i].astype(F32) for i in range(8)])
        for t in range(8):
            flat[tile_a * 8 + t, :, h * L : (h + 1) * L] = xs[t].astype(BF16)
    for t in range(8):
        flat[8 + t] = flat_in[8 + t]
        flat[tile_b * 8 + t] = flat_in[tile_b * 8 + t]

    def operators():
        totals[...] = jnp.zeros(totals.shape, F32)
        for k in range(KDEV):
            contrib[k] = jnp.dot(flat[col_ids[k]], blocks[k], preferred_element_type=F32)
        for k in range(KDEV):
            r = row_ids[k]
            totals[r] = totals[r] + contrib[k]
        for r in range(RB):
            seen = vis[r]
            moved = v[r] + 0.5 * totals[r]
            offset = 2.0 * moved - seen
            length = jnp.sqrt(
                jnp.sum(jnp.sum(offset * offset, axis=1, keepdims=True), axis=0, keepdims=True)
            )
            radius = radii[0:1, r : r + 1]
            scale = radius / jnp.maximum(length, radius)
            new = moved - 0.5 * (seen + offset * scale)
            v_out[r] = new
            if not last:
                vb[r] = new.astype(BF16)
        if last:
            put = pltpu.make_async_copy(v_out, v_hbm, out_sems.at[NB])
            put.start()
            puts.append(put)
        else:
            back_project(vb, blocks_turned, False, row_ids, col_ids, tiles, sums)

    def filtered(t, b):
        cols = slice(b * L, (b + 1) * L)
        if t < W:
            return wide[t * C : (t + 1) * C, cols]
        if t < W + R:
            return inner[(t - W) * C : (t - W + 1) * C, cols]
        return wide[(t - R) * C : (t - R + 1) * C, cols]

    def wavelets(bases):
        for b in bases:
            rows = []
            for r in range(R):
                if W <= r < R - W:
                    total = middle[b, (r - W) * C : (r - W + 1) * C, :]
                else:
                    total = filter_row(row_taps, b, [(a, filtered(r + a, b)) for a in range(TAPS)])
                full = u_rows[b, r * C : (r + 1) * C, :].astype(F32) + 0.5 * total
                size = jnp.sqrt(jnp.sum(full * full, axis=0, keepdims=True))
                limit = thr[b, r : r + 1, :]
                new = full * (limit / jnp.maximum(size, limit))
                if last:
                    turned[b, r * C : (r + 1) * C, :] = new
                else:
                    new = new.astype(BF16)
                    u_out[b, r * C : (r + 1) * C, :] = new
                    rows.append(new.astype(F32))
            if last:
                for c in range(C):
                    u_out[b, c * R : (c + 1) * R, :] = turned[b, pl.ds(c, R, stride=C), :].astype(BF16)
                put = pltpu.make_async_copy(u_out.at[b], u_hbm.at[b], out_sems.at[b])
                put.start()
                puts.append(put)
            else:
                synth_rows(row_taps, b, rows, wide_next)

    wavelets(range(NB))
    get_rows.wait()
    get_cols.wait()
    operators()
    for put in puts:
        put.wait()
    if not last:
        make_message(sums, wide_next, col_h, col_l, smooth, msg)


def shape(dims, dtype=F32):
    return jax.ShapeDtypeStruct(dims, dtype)


def scratch(*dims, dtype=F32):
    return pltpu.VMEM(dims, dtype)


def small(dims, dtype):
    return pltpu.SMEM(dims, dtype)


HALF = [shape((NT3, C, VB)), shape((RE * C, NB * L), BF16), shape((R + 1, C, L), BF16)]


def call(kernel, far, arrays, outs, temps=(), name=None, mib=8, final=0):
    far = [pltpu.with_memory_space_constraint(a, pltpu.HBM) for a in far]
    arrays = [pltpu.with_memory_space_constraint(a, pltpu.VMEM) for a in arrays]
    anywhere = pl.BlockSpec(memory_space=pl.ANY)
    return pl.pallas_call(
        kernel,
        out_shape=tuple(
            (pltpu.HBM if i < final else pltpu.VMEM)(o.shape, o.dtype) for i, o in enumerate(outs)
        ),
        in_specs=[anywhere] * len(far) + [VMEM] * len(arrays),
        out_specs=tuple(anywhere if i < final else VMEM for i in range(len(outs))),
        scratch_shapes=list(temps),
        compiler_params=pltpu.CompilerParams(vmem_limit_bytes=mib << 20),
        name=name,
    )(*far, *arrays)


def pairs_of(axis):
    count = lax.axis_size(axis)
    inner = [(i, i ^ 1) for i in range(count)]
    outer = [(i, ((i + 1) ^ 1) - 1) for i in range(1, count - 1)]
    return inner, outer


def per_device(
    image, wavelet_dual, thresholds, filter_taps, visibilities,
    data_dual, ball_radii, blocks, row_index, col_index,
):
    image_rows = image.reshape(C * R, L)
    u = wavelet_dual.reshape(NB, C * R, L)
    seen, v = visibilities[0, 0], data_dual[0, 0]
    radii, row_ids, col_ids = ball_radii[0], row_index[0, 0], col_index[0, 0]
    taps = filter_taps.transpose(2, 1, 0)
    facet_in, facet_out = pairs_of("facet")
    grp_in, grp_out = pairs_of("grp")
    scalars = [small((KDEV,), jnp.int32), small((KDEV,), jnp.int32)]
    sums, wide_rows, msg, u, col_h, col_l, operators, row_taps = call(
        first_kernel,
        (taps, row_ids, col_ids, u, v, blocks[0, 0]),
        (),
        HALF
        + [
            shape((NB, R * C, L), BF16),
            shape((NB * L, 2 * L), BF16),
            shape((NB * L, 2 * L), BF16),
            shape((KDEV, VB, VB), BF16),
            shape((TAPS, NB, C // 2, L)),
        ],
        scalars
        + [
            scratch(TAPS, 2, NB),
            scratch(TAPS, NB, C // 2, L),
            scratch(NB, C * R, L, dtype=BF16),
            scratch(RB, C, VB),
            scratch(RB, C, VB, dtype=BF16),
            scratch(KDEV, C, VB),
            scratch(NB, C * R, L),
            scratch(W * C, 2 * L),
            pltpu.SemaphoreType.DMA((6,)),
        ],
        name="first",
        mib=16,
    )
    x = x_ext = None
    for iteration in range(ITERS):
        first, last = iteration == 0, iteration == ITERS - 1
        got = lax.ppermute(msg, "facet", facet_in)
        main, ext = call(
            sums_kernel,
            (),
            (sums, wide_rows, col_h, col_l),
            [shape((BAND, C, L)), shape((RE, C, L))],
            [scratch(RE * C, 2 * L)],
            name="sums",
        )
        total, total_ext, msg = call(
            lambda *refs: pair_kernel(first, *refs),
            (),
            (main, ext, got) + ((image_rows,) if first else ()),
            [
                shape((R, C, L)),
                shape((R, C, L)),
                shape(((3 if first else 2) * R + 2, C, L), BF16),
            ],
            name="pair",
        )
        got = lax.ppermute(msg, "facet", facet_out)
        if first:
            (turned,) = call(
                turn_kernel, (), (operators, total), [shape((KDEV, VB, VB), BF16)], name="turn", mib=4
            )
        rim = shape((4 if first else 2, C, L), BF16)
        part, part_ext, msg_a, msg_b, *rest = call(
            lambda *refs: rim_kernel(first, *refs),
            (),
            (total, total_ext, main, ext, got) + ((image_rows, turned) if first else ()),
            [shape((2 * R, C, L)), shape((2 * R, C, L)), rim, rim]
            + ([shape((2 * R, C, L))] if first else []),
            name="rim",
        )
        if first:
            x = rest[0]
        got_a = lax.ppermute(msg_a, "grp", grp_in)
        got_b = lax.ppermute(msg_b, "grp", grp_out)
        wide = shape((2 * R, C, L))
        outs = [shape((2 * R, C, L), BF16), shape((2 * R, C, L), BF16), shape((R + 1, C, L), BF16)]
        results = call(
            lambda *refs: primal_kernel(first, last, *refs),
            (),
            (part, part_ext, got_a, got_b, x) + (() if first else (x_ext,)),
            ([shape((C * R, L))] if last else [wide, wide]) + outs,
            [scratch(R * C, L)] if last else [],
            name="primal",
        )
        e, e_ext, msg = results[-3:]
        if last:
            image_out = results[0]
        else:
            x, x_ext = results[:2]
        got = lax.ppermute(msg, "facet", facet_in)
        flat, inner, edge, middle = call(
            near_kernel,
            (),
            (e, e_ext, col_h, col_l, row_taps),
            [
                shape((NT3, C, VB), BF16),
                shape((R * C, NB * L)),
                shape((W * C, 2 * L), BF16),
                shape((NB, (R - 2 * W) * C, L)),
            ],
            name="near",
        )
        outs = [shape((RB, C, VB)), shape((NB, R * C, L), BF16)]
        if last:
            outs = [shape((C * R, L))] + outs
            temps = [
                scratch(RB, C, VB),
                scratch(NB, C * R, L, dtype=BF16),
                scratch(NB, R * C, L),
                pltpu.SemaphoreType.DMA((NB + 2,)),
            ]
        else:
            temps = [scratch(RB, C, VB, dtype=BF16), scratch(KDEV, C, VB), scratch(W * C, 2 * L)]
        *half, v, u = call(
            lambda *refs: dual_kernel(last, *refs),
            (),
            (flat, inner, edge, middle, got, v, seen, operators, u, thresholds, col_h, col_l)
            + (row_taps, radii, row_ids, col_ids)
            + ((image_out,) if last else (turned,)),
            ([] if last else HALF) + outs,
            temps
            + scalars
            + [
                pltpu.SemaphoreType.DMA((2,)),
                scratch(NT3, C, VB, dtype=BF16),
                scratch(2 * W * C, NB * L),
                scratch(2, W * C, 2 * L, dtype=BF16),
                scratch(KDEV, C, VB),
                scratch(RB, C, VB),
            ],
            name="dual",
            mib=16,
            final=3 if last else 0,
        )
        if last:
            (image_out,) = half
        else:
            sums, wide_rows, msg = half
    return (image_out.reshape(C, R, L), v[None, None], u.reshape(NB, C, R, L))


def solution(mesh):
    in_specs = (
        P(None, "facet", "grp"),
        P(None, None, "facet", "grp"),
        P(None, "facet", "grp"),
        P(),
        P("facet", "grp", None, None, None),
        P("facet", "grp", None, None, None),
        P("facet", "grp", None),
        P("facet", "grp", None, None, None),
        P("facet", "grp", None),
        P("facet", "grp", None),
    )
    out_specs = (
        P(None, "facet", "grp"),
        P("facet", "grp", None, None, None),
        P(None, None, "facet", "grp"),
    )
    return jax.shard_map(
        per_device, mesh=mesh, in_specs=in_specs, out_specs=out_specs, check_vma=False
    )
```

```python
import jax
import jax.numpy as jnp
from jax import lax
from jax.experimental import pallas as pl
from jax.experimental.pallas import tpu as pltpu
from jax.sharding import PartitionSpec as P

ITERS = 2
NB = 8
C = 16
R = 16
L = 128
W = 3
TAPS = 7
RB = 8
KDEV = 16
NT3 = 24
VB = 256
RE = R + 2 * W
BAND = 3 * R
F32 = jnp.float32
BF16 = jnp.bfloat16

VMEM = pl.BlockSpec(memory_space=pltpu.VMEM)


def lanes():
    return lax.broadcasted_iota(jnp.int32, (C, L), 1)


def roll(x, shift):
    shift = shift % L
    return x if shift == 0 else pltpu.roll(x, shift, 1)


def is_odd(axis):
    return lax.rem(lax.axis_index(axis), 2) == 1


def pack(rows):
    total = rows[0]
    for i in range(1, len(rows)):
        total = total + roll(rows[i], 8 * i)
    return total


def unpack(packed, i, lane):
    return jnp.where(lane < 6, roll(packed, -8 * i), 0.0)


def swap_blocks(xs):
    xs = list(xs)
    lane = lanes()
    for bit in range(3):
        m = 1 << bit
        low = (lane // (16 * m)) % 2 == 0
        for i in range(8):
            if i & m == 0:
                a, b = xs[i], xs[i | m]
                xs[i] = jnp.where(low, a, roll(b, 16 * m))
                xs[i | m] = jnp.where(low, roll(a, -16 * m), b)
    return xs


def build_columns(col_taps, high, low):
    strip = 8
    for start in range(0, L, strip):
        j = start + lax.broadcasted_iota(jnp.int32, (strip, L), 0)
        n = lax.broadcasted_iota(jnp.int32, (strip, L), 1)
        outside = jnp.where(n < W, n - W, jnp.where(n < 2 * W, n - W + L, 2 * L))
        edge = start == 0 or start == L - strip
        for tile, place in ((0, n), (1, outside)):
            tap = place - j + W
            for b in range(NB):
                value = jnp.zeros((strip, L), F32)
                if tile == 0 or edge:
                    for e in range(TAPS):
                        value = jnp.where(tap == e, col_taps[e, b], value)
                rounded = value.astype(BF16)
                rows, cols = slice(b * L + start, b * L + start + strip), slice(tile * L, (tile + 1) * L)
                high[rows, cols] = rounded
                low[rows, cols] = (value - rounded.astype(F32)).astype(BF16)


def times(tap, row):
    return (tap[None] * row.reshape(2, C // 2, L)).reshape(C, L)


def filter_row(row_taps, b, terms):
    total = None
    for a, row in terms:
        term = times(row_taps[a, b], row)
        total = term if total is None else total + term
    return total


def back_project(vb, blocks, across, row_ids, col_ids, contrib, sums):
    sums[...] = jnp.zeros(sums.shape, F32)
    for k in range(KDEV):
        contrib[k] = lax.dot_general(
            vb[row_ids[k]], blocks[k], (((1,), (int(across),)), ((), ())), preferred_element_type=F32
        )
    for k in range(KDEV):
        q = col_ids[k]
        sums[q] = sums[q] + contrib[k]


def turn_kernel(blocks, after, turned):
    for k in range(KDEV):
        turned[k] = blocks[k].T


def synth_rows(row_taps, b, rows, places, wide_h, wide_l):
    for spot, i in enumerate(places):
        terms = [(a, rows[i - a]) for a in range(TAPS) if 0 <= i - a < R]
        total = filter_row(row_taps, b, terms)
        high = total.astype(BF16)
        wide_h[spot * C : (spot + 1) * C, b * L : (b + 1) * L] = high
        wide_l[spot * C : (spot + 1) * C, b * L : (b + 1) * L] = (total - high.astype(F32)).astype(BF16)


OUTER = tuple(range(W)) + tuple(range(R + W, RE))


def filter_columns(rows_h, rows_l, col_h, col_l):
    return (
        jnp.dot(rows_h, col_h[...], preferred_element_type=F32)
        + jnp.dot(rows_l, col_h[...], preferred_element_type=F32)
        + jnp.dot(rows_h, col_l[...], preferred_element_type=F32)
    )


def make_message(sums, wide_h, wide_l, col_h, col_l, smooth, msg):
    odd = is_odd("facet")
    tile_row = jnp.where(odd, 0, 2)
    top = pl.multiple_of(jnp.where(odd, 0, W * C), C)
    smooth[...] = filter_columns(
        wide_h[pl.ds(top, W * C), :], wide_l[pl.ds(top, W * C), :], col_h, col_l
    )
    for h in range(2):
        xs = swap_blocks([sums[tile_row * 8 + t, :, h * L : (h + 1) * L] for t in range(8)])
        for i in range(8):
            r = h * 8 + i
            value = xs[i]
            if r < W:
                value = value + jnp.where(odd, 0.0, smooth[r * C : (r + 1) * C, :L])
            if r >= R - W:
                t = r - (R - W)
                value = value + jnp.where(odd, smooth[t * C : (t + 1) * C, :L], 0.0)
            msg[r] = value.astype(BF16)
    msg[R] = pack([smooth[i * C : (i + 1) * C, L:] for i in range(W)]).astype(BF16)


def sums_kernel(sums, u_rows, row_taps, col_h, col_l, main, ext, smooth, wide_h, wide_l):
    for b in range(NB):
        rows = [u_rows[b, r * C : (r + 1) * C, :].astype(F32) for r in range(R)]
        synth_rows(row_taps, b, rows, range(RE), wide_h, wide_l)
    smooth[...] = filter_columns(wide_h[...], wide_l[...], col_h, col_l)
    for tr in range(3):
        for h in range(2):
            xs = swap_blocks([sums[tr * 8 + t, :, h * L : (h + 1) * L] for t in range(8)])
            for i in range(8):
                r = tr * R + h * 8 + i
                t = r - (R - W)
                value = xs[i]
                if 0 <= t < RE:
                    value = value + smooth[t * C : (t + 1) * C, :L]
                main[r] = value
    for t in range(RE):
        ext[t] = smooth[t * C : (t + 1) * C, L:]


def fetch(sources, targets, sems):
    copies = [pltpu.make_async_copy(s, t, sems.at[i]) for i, (s, t) in enumerate(zip(sources, targets))]
    for copy in copies:
        copy.start()
    return copies


def first_kernel(
    taps_hbm, rows_hbm, cols_hbm, u_hbm, v_hbm, blocks_hbm,
    sums, msg, u_rows, col_h, col_l, blocks, row_taps,
    row_ids, col_ids, taps, col_taps, u, v, vb, contrib, turned, smooth, wide_h, wide_l, sems,
):
    get_u, get_taps, get_v, get_blocks, get_rows, get_cols = fetch(
        (u_hbm, taps_hbm, v_hbm, blocks_hbm, rows_hbm, cols_hbm),
        (u, taps, v, blocks, row_ids, col_ids),
        sems,
    )
    get_taps.wait()
    for a in range(TAPS):
        for b in range(NB):
            row_taps[a, b] = jnp.broadcast_to(taps[a, 0:1, b : b + 1], (C // 2, L))
            col_taps[a, b] = jnp.broadcast_to(taps[a, 1:2, b : b + 1], (C // 2, L))
    get_u.wait()
    for b in range(NB):
        turned[b] = u[b].astype(F32)
    build_columns(col_taps, col_h, col_l)

    def wavelets(b):
        rows = [turned[b, pl.ds(r, C, stride=R), :] for r in range(R)]
        for r in range(R):
            u_rows[b, r * C : (r + 1) * C, :] = rows[r].astype(BF16)
        synth_rows(row_taps, b, rows, OUTER, wide_h, wide_l)

    for b in range(NB):
        wavelets(b)
    get_v.wait()
    get_rows.wait()
    get_cols.wait()
    get_blocks.wait()
    vb[...] = v[...].astype(BF16)
    back_project(vb, blocks, True, row_ids, col_ids, contrib, sums)
    make_message(sums, wide_h, wide_l, col_h, col_l, smooth, msg)


def pair_kernel(with_image, *refs):
    if with_image:
        main, ext, got, image, total, total_ext, msg = refs
    else:
        main, ext, got, total, total_ext, msg = refs
    odd = is_odd("facet")
    lane = lanes()
    for r in range(R):
        row = main[R + r] + got[r].astype(F32)
        total[r] = row
        msg[R + r] = row.astype(BF16)
        total_ext[r] = ext[W + r]
    spot = jnp.where(odd, 0, R - W)
    packed = got[R].astype(F32)
    for i in range(W):
        total_ext[spot + i] = total_ext[spot + i] + unpack(packed, i, lane)
    far = jnp.where(odd, 2 * R, 0)
    far_ext = jnp.where(odd, R + W, 0)
    for r in range(R):
        msg[r] = main[far + r].astype(BF16)
    msg[2 * R] = pack([total_ext[r] for r in range(R)]).astype(BF16)
    msg[2 * R + 1] = pack([ext[far_ext + i] for i in range(W)]).astype(BF16)
    if with_image:
        for r in range(R):
            msg[2 * R + 2 + r] = image[pl.ds(r, C, stride=R), :].astype(BF16)


def rim_kernel(with_image, *refs):
    if with_image:
        total, total_ext, main, ext, got, image, _, part, part_ext, msg_a, msg_b, x = refs
    else:
        total, total_ext, main, ext, got, part, part_ext, msg_a, msg_b = refs
    odd = is_odd("facet")
    lane = lanes()
    far = jnp.where(odd, 2 * R, 0)
    far_ext = jnp.where(odd, R + W, 0)
    packed = got[2 * R].astype(F32)
    for r in range(R):
        part[r] = total[r] + got[r].astype(F32)
        part_ext[r] = total_ext[r]
        part[R + r] = got[R + r].astype(F32) + main[far + r]
        part_ext[R + r] = unpack(packed, r, lane)
    near = jnp.where(odd, R - W, 0)
    away = jnp.where(odd, 0, R - W)
    packed = got[2 * R + 1].astype(F32)
    for i in range(W):
        part_ext[near + i] = part_ext[near + i] + unpack(packed, i, lane)
        part_ext[R + away + i] = part_ext[R + away + i] + ext[far_ext + i]
    if with_image:
        for r in range(R):
            x[r] = image[pl.ds(r, C, stride=R), :]
            x[R + r] = got[2 * R + 2 + r].astype(F32)
    godd = is_odd("grp")
    slot = lane // 8
    sub = lane % 8
    first = sub < W
    second = (sub >= W) & (sub < 2 * W)
    for p in range(2):
        left = jnp.zeros((C, L), F32)
        right = jnp.zeros((C, L), F32)
        for r in range(R):
            row, row_ext = part[p * R + r], part_ext[p * R + r]
            one = (slot == r) & first
            two = (slot == r) & second
            left = jnp.where(one, roll(row_ext, 8 * r), left)
            left = jnp.where(two, roll(row, 8 * r + W), left)
            right = jnp.where(one, roll(row_ext, 8 * r - W), right)
            right = jnp.where(two, roll(row, 8 * r + 2 * W), right)
        msg_a[p] = jnp.where(godd, left, right).astype(BF16)
        msg_b[p] = jnp.where(godd, right, left).astype(BF16)
        if with_image:
            left = jnp.zeros((C, L), F32)
            right = jnp.zeros((C, L), F32)
            for r in range(R):
                row = x[p * R + r]
                one = (slot == r) & first
                left = jnp.where(one, roll(row, 8 * r), left)
                right = jnp.where(one, roll(row, 8 * r + W), right)
            msg_a[2 + p] = jnp.where(godd, left, right).astype(BF16)
            msg_b[2 + p] = jnp.where(godd, right, left).astype(BF16)


def primal_kernel(first, last, *refs):
    refs = list(refs)
    part, part_ext, got_a, got_b, x = refs[:5]
    refs = refs[5:]
    if not first:
        x_ext = refs.pop(0)
    if last:
        image_out, e, e_ext, msg, turned = refs
    else:
        new_x, new_x_ext, e, e_ext, msg = refs
    lane = lanes()
    facet, grp = lax.axis_index("facet"), lax.axis_index("grp")
    odd = is_odd("facet")
    godd = is_odd("grp")
    on_left = (grp > 0) & (lane < W)
    on_right = (grp < lax.axis_size("grp") - 1) & (lane >= W) & (lane < 2 * W)
    inside = on_left | on_right
    there = jnp.where(odd, facet < lax.axis_size("facet") - 1, facet > 0)
    got_a_wide = got_a[...].astype(F32)
    got_b_wide = got_b[...].astype(F32)
    from_left = jnp.where(godd, got_a_wide, got_b_wide)
    from_right = jnp.where(godd, got_b_wide, got_a_wide)
    rims = []
    for p in range(2):
        for r in range(R):
            i = p * R + r
            grad = part[i] + jnp.where(lane < W, roll(from_left[p], -8 * r), 0.0)
            grad = grad + jnp.where(lane >= L - W, roll(from_right[p], -8 * r - W), 0.0)
            rim = jnp.where(
                lane < W, roll(from_left[p], -8 * r - W), roll(from_right[p], -8 * r)
            )
            grad_ext = part_ext[i] + rim
            old = x[i]
            if first:
                old_ext = jnp.where(
                    lane < W, roll(from_left[2 + p], -8 * r), roll(from_right[2 + p], -8 * r + W)
                )
            else:
                old_ext = x_ext[i]
            new = jnp.maximum(old - 0.5 * grad, 0.0)
            new_ext = jnp.maximum(old_ext - 0.5 * grad_ext, 0.0)
            ahead = 2.0 * new - old
            ahead_ext = jnp.where(inside, 2.0 * new_ext - old_ext, 0.0)
            if p == 1:
                ahead = jnp.where(there, ahead, 0.0)
                ahead_ext = jnp.where(there, ahead_ext, 0.0)
            e[i] = ahead.astype(BF16)
            e_ext[i] = ahead_ext.astype(BF16)
            if p == 0:
                msg[r] = ahead.astype(BF16)
                rims.append(ahead_ext)
                if last:
                    turned[r * C : (r + 1) * C, :] = new
            if not last:
                new_x[i] = new
                new_x_ext[i] = new_ext
    msg[R] = pack(rims).astype(BF16)
    if last:
        for c in range(C):
            image_out[c * R : (c + 1) * R, :] = turned[pl.ds(c, R, stride=C), :]


def shrunk(u_row, coefficient, limit):
    full = u_row.astype(F32) + 0.5 * coefficient
    size = jnp.sqrt(jnp.sum(full * full, axis=0, keepdims=True))
    return full * (limit / jnp.maximum(size, limit))


def near_kernel(e, e_ext, col_h, col_l, row_taps, u_rows, thr, flat, wide, edge, middle):
    odd = is_odd("facet")
    base_b = jnp.where(odd, 2, 0)
    for tile_row, base in ((1, 0), (base_b, R)):
        for h in range(2):
            xs = swap_blocks([e[base + h * 8 + i].astype(F32) for i in range(8)])
            for t in range(8):
                flat[tile_row * 8 + t, :, h * L : (h + 1) * L] = xs[t].astype(BF16)
    near = jnp.concatenate([e[:R].reshape(R * C, L), e_ext[:R].reshape(R * C, L)], axis=1)
    wide[...] = spread_columns(near, col_h, col_l)
    start = jnp.where(odd, R, 2 * R - W)
    for i in range(W):
        edge[i * C : (i + 1) * C, :L] = e[start + i]
        edge[i * C : (i + 1) * C, L:] = e_ext[start + i]
    for b in range(NB):
        cols = slice(b * L, (b + 1) * L)
        for r in range(W, R - W):
            terms = [(a, wide[(r - W + a) * C : (r - W + a + 1) * C, cols]) for a in range(TAPS)]
            new = shrunk(
                u_rows[b, r * C : (r + 1) * C, :], filter_row(row_taps, b, terms), thr[b, r : r + 1, :]
            )
            middle[b, (r - W) * C : (r - W + 1) * C, :] = new.astype(BF16)


def spread_columns(rows, col_h, col_l):
    both = (((1,), (1,)), ((), ()))
    return lax.dot_general(rows, col_h[...], both, preferred_element_type=F32) + lax.dot_general(
        rows, col_l[...], both, preferred_element_type=F32
    )


def dual_kernel(last, *refs):
    flat_in, inner, edge, middle, got, v, vis, blocks, u_rows, thr, col_h, col_l = refs[:12]
    row_taps, radii, rows_vmem, cols_vmem = refs[12:16]
    refs = refs[16:]
    if last:
        image, image_hbm, v_hbm, u_hbm, *refs = refs
        v_out, u_out, turned, out_sems, *refs = refs
    else:
        blocks_turned, sums, msg, v_out, u_out, *refs = refs
        vb, tiles, smooth, wide_h, wide_l, *refs = refs
    row_ids, col_ids, sems, flat, wide, edges, contrib, totals = refs
    get_rows, get_cols = fetch((rows_vmem, cols_vmem), (row_ids, col_ids), sems)
    puts = []
    if last:
        put = pltpu.make_async_copy(image, image_hbm, out_sems.at[NB + 1])
        put.start()
        puts.append(put)
    odd = is_odd("facet")
    lane = lanes()
    packed = got[R].astype(F32)
    near_a = jnp.where(odd, R - W, 0)
    above, below = edges.at[0], edges.at[1]
    for i in range(W):
        rows = slice(i * C, (i + 1) * C)
        mine = edge[rows, :]
        rim = jnp.where(odd, roll(packed, -8 * (R - W + i)), roll(packed, -8 * i))
        theirs = jnp.concatenate(
            [got[near_a + i], jnp.where(lane < 2 * W, rim, 0.0).astype(BF16)], axis=1
        )
        above[rows, :] = jnp.where(odd, theirs, mine)
        below[rows, :] = jnp.where(odd, mine, theirs)
    wide[: W * C, :] = spread_columns(above[...], col_h, col_l)
    wide[W * C :, :] = spread_columns(below[...], col_h, col_l)
    tile_a = jnp.where(odd, 0, 2)
    tile_b = jnp.where(odd, 2, 0)
    for h in range(2):
        xs = swap_blocks([got[h * 8 + i].astype(F32) for i in range(8)])
        for t in range(8):
            flat[tile_a * 8 + t, :, h * L : (h + 1) * L] = xs[t].astype(BF16)
    for t in range(8):
        flat[8 + t] = flat_in[8 + t]
        flat[tile_b * 8 + t] = flat_in[tile_b * 8 + t]

    def operators():
        totals[...] = jnp.zeros(totals.shape, F32)
        for k in range(KDEV):
            contrib[k] = jnp.dot(flat[col_ids[k]], blocks[k], preferred_element_type=F32)
        for k in range(KDEV):
            r = row_ids[k]
            totals[r] = totals[r] + contrib[k]
        for r in range(RB):
            seen = vis[r]
            moved = v[r] + 0.5 * totals[r]
            offset = 2.0 * moved - seen
            length = jnp.sqrt(
                jnp.sum(jnp.sum(offset * offset, axis=1, keepdims=True), axis=0, keepdims=True)
            )
            radius = radii[0:1, r : r + 1]
            scale = radius / jnp.maximum(length, radius)
            new = moved - 0.5 * (seen + offset * scale)
            v_out[r] = new
            if not last:
                vb[r] = new.astype(BF16)
        if last:
            put = pltpu.make_async_copy(v_out, v_hbm, out_sems.at[NB])
            put.start()
            puts.append(put)
        else:
            back_project(vb, blocks_turned, False, row_ids, col_ids, tiles, sums)

    def filtered(t, b):
        cols = slice(b * L, (b + 1) * L)
        if t < W:
            return wide[t * C : (t + 1) * C, cols]
        if t < W + R:
            return inner[(t - W) * C : (t - W + 1) * C, cols]
        return wide[(t - R) * C : (t - R + 1) * C, cols]

    def wavelets(bases):
        for b in bases:
            rows = []
            for r in range(R):
                if W <= r < R - W:
                    new = middle[b, (r - W) * C : (r - W + 1) * C, :]
                else:
                    new = shrunk(
                        u_rows[b, r * C : (r + 1) * C, :],
                        filter_row(row_taps, b, [(a, filtered(r + a, b)) for a in range(TAPS)]),
                        thr[b, r : r + 1, :],
                    ).astype(BF16)
                if last:
                    turned[b, r * C : (r + 1) * C, :] = new.astype(F32)
                else:
                    u_out[b, r * C : (r + 1) * C, :] = new
                    rows.append(new.astype(F32))
            if last:
                for c in range(C):
                    u_out[b, c * R : (c + 1) * R, :] = turned[b, pl.ds(c, R, stride=C), :].astype(BF16)
                put = pltpu.make_async_copy(u_out.at[b], u_hbm.at[b], out_sems.at[b])
                put.start()
                puts.append(put)
            else:
                synth_rows(row_taps, b, rows, OUTER, wide_h, wide_l)

    wavelets(range(NB))
    get_rows.wait()
    get_cols.wait()
    operators()
    for put in puts:
        put.wait()
    if not last:
        make_message(sums, wide_h, wide_l, col_h, col_l, smooth, msg)


def shape(dims, dtype=F32):
    return jax.ShapeDtypeStruct(dims, dtype)


def scratch(*dims, dtype=F32):
    return pltpu.VMEM(dims, dtype)


def small(dims, dtype):
    return pltpu.SMEM(dims, dtype)


HALF = [shape((NT3, C, VB)), shape((R + 1, C, L), BF16)]
OUTER_TEMPS = [
    scratch(2 * W * C, NB * L, dtype=BF16),
    scratch(2 * W * C, NB * L, dtype=BF16),
]


def call(kernel, far, arrays, outs, temps=(), name=None, mib=8, final=0):
    far = [pltpu.with_memory_space_constraint(a, pltpu.HBM) for a in far]
    arrays = [pltpu.with_memory_space_constraint(a, pltpu.VMEM) for a in arrays]
    anywhere = pl.BlockSpec(memory_space=pl.ANY)
    return pl.pallas_call(
        kernel,
        out_shape=tuple(
            (pltpu.HBM if i < final else pltpu.VMEM)(o.shape, o.dtype) for i, o in enumerate(outs)
        ),
        in_specs=[anywhere] * len(far) + [VMEM] * len(arrays),
        out_specs=tuple(anywhere if i < final else VMEM for i in range(len(outs))),
        scratch_shapes=list(temps),
        compiler_params=pltpu.CompilerParams(vmem_limit_bytes=mib << 20),
        name=name,
    )(*far, *arrays)


def pairs_of(axis):
    count = lax.axis_size(axis)
    inner = [(i, i ^ 1) for i in range(count)]
    outer = [(i, ((i + 1) ^ 1) - 1) for i in range(1, count - 1)]
    return inner, outer


def per_device(
    image, wavelet_dual, thresholds, filter_taps, visibilities,
    data_dual, ball_radii, blocks, row_index, col_index,
):
    image_rows = image.reshape(C * R, L)
    u = wavelet_dual.reshape(NB, C * R, L)
    seen, v = visibilities[0, 0], data_dual[0, 0]
    radii, row_ids, col_ids = ball_radii[0], row_index[0, 0], col_index[0, 0]
    taps = filter_taps.transpose(2, 1, 0)
    facet_in, facet_out = pairs_of("facet")
    grp_in, grp_out = pairs_of("grp")
    scalars = [small((KDEV,), jnp.int32), small((KDEV,), jnp.int32)]
    sums, msg, u, col_h, col_l, operators, row_taps = call(
        first_kernel,
        (taps, row_ids, col_ids, u, v, blocks[0, 0]),
        (),
        HALF
        + [
            shape((NB, R * C, L), BF16),
            shape((NB * L, 2 * L), BF16),
            shape((NB * L, 2 * L), BF16),
            shape((KDEV, VB, VB), BF16),
            shape((TAPS, NB, C // 2, L)),
        ],
        scalars
        + [
            scratch(TAPS, 2, NB),
            scratch(TAPS, NB, C // 2, L),
            scratch(NB, C * R, L, dtype=BF16),
            scratch(RB, C, VB),
            scratch(RB, C, VB, dtype=BF16),
            scratch(KDEV, C, VB),
            scratch(NB, C * R, L),
            scratch(W * C, 2 * L),
            *OUTER_TEMPS,
            pltpu.SemaphoreType.DMA((6,)),
        ],
        name="first",
        mib=16,
    )
    x = x_ext = None
    for iteration in range(ITERS):
        first, last = iteration == 0, iteration == ITERS - 1
        got = lax.ppermute(msg, "facet", facet_in)
        main, ext = call(
            sums_kernel,
            (),
            (sums, u, row_taps, col_h, col_l),
            [shape((BAND, C, L)), shape((RE, C, L))],
            [
                scratch(RE * C, 2 * L),
                scratch(RE * C, NB * L, dtype=BF16),
                scratch(RE * C, NB * L, dtype=BF16),
            ],
            name="sums",
        )
        total, total_ext, msg = call(
            lambda *refs: pair_kernel(first, *refs),
            (),
            (main, ext, got) + ((image_rows,) if first else ()),
            [
                shape((R, C, L)),
                shape((R, C, L)),
                shape(((3 if first else 2) * R + 2, C, L), BF16),
            ],
            name="pair",
        )
        got = lax.ppermute(msg, "facet", facet_out)
        if first:
            (turned,) = call(
                turn_kernel, (), (operators, total), [shape((KDEV, VB, VB), BF16)], name="turn", mib=4
            )
        rim = shape((4 if first else 2, C, L), BF16)
        part, part_ext, msg_a, msg_b, *rest = call(
            lambda *refs: rim_kernel(first, *refs),
            (),
            (total, total_ext, main, ext, got) + ((image_rows, turned) if first else ()),
            [shape((2 * R, C, L)), shape((2 * R, C, L)), rim, rim]
            + ([shape((2 * R, C, L))] if first else []),
            name="rim",
        )
        if first:
            x = rest[0]
        got_a = lax.ppermute(msg_a, "grp", grp_in)
        got_b = lax.ppermute(msg_b, "grp", grp_out)
        wide = shape((2 * R, C, L))
        outs = [shape((2 * R, C, L), BF16), shape((2 * R, C, L), BF16), shape((R + 1, C, L), BF16)]
        results = call(
            lambda *refs: primal_kernel(first, last, *refs),
            (),
            (part, part_ext, got_a, got_b, x) + (() if first else (x_ext,)),
            ([shape((C * R, L))] if last else [wide, wide]) + outs,
            [scratch(R * C, L)] if last else [],
            name="primal",
        )
        e, e_ext, msg = results[-3:]
        if last:
            image_out = results[0]
        else:
            x, x_ext = results[:2]
        got = lax.ppermute(msg, "facet", facet_in)
        flat, inner, edge, middle = call(
            near_kernel,
            (),
            (e, e_ext, col_h, col_l, row_taps, u, thresholds),
            [
                shape((NT3, C, VB), BF16),
                shape((R * C, NB * L)),
                shape((W * C, 2 * L), BF16),
                shape((NB, (R - 2 * W) * C, L), BF16),
            ],
            name="near",
        )
        outs = [shape((RB, C, VB)), shape((NB, R * C, L), BF16)]
        if last:
            outs = [shape((C * R, L))] + outs
            temps = [
                scratch(RB, C, VB),
                scratch(NB, C * R, L, dtype=BF16),
                scratch(NB, R * C, L),
                pltpu.SemaphoreType.DMA((NB + 2,)),
            ]
        else:
            temps = [
                scratch(RB, C, VB, dtype=BF16),
                scratch(KDEV, C, VB),
                scratch(W * C, 2 * L),
                *OUTER_TEMPS,
            ]
        *half, v, u = call(
            lambda *refs: dual_kernel(last, *refs),
            (),
            (flat, inner, edge, middle, got, v, seen, operators, u, thresholds, col_h, col_l)
            + (row_taps, radii, row_ids, col_ids)
            + ((image_out,) if last else (turned,)),
            ([] if last else HALF) + outs,
            temps
            + scalars
            + [
                pltpu.SemaphoreType.DMA((2,)),
                scratch(NT3, C, VB, dtype=BF16),
                scratch(2 * W * C, NB * L),
                scratch(2, W * C, 2 * L, dtype=BF16),
                scratch(KDEV, C, VB),
                scratch(RB, C, VB),
            ],
            name="dual",
            mib=16,
            final=3 if last else 0,
        )
        if last:
            (image_out,) = half
        else:
            sums, msg = half
    return (image_out.reshape(C, R, L), v[None, None], u.reshape(NB, C, R, L))


def solution(mesh):
    in_specs = (
        P(None, "facet", "grp"),
        P(None, None, "facet", "grp"),
        P(None, "facet", "grp"),
        P(),
        P("facet", "grp", None, None, None),
        P("facet", "grp", None, None, None),
        P("facet", "grp", None),
        P("facet", "grp", None, None, None),
        P("facet", "grp", None),
        P("facet", "grp", None),
    )
    out_specs = (
        P(None, "facet", "grp"),
        P("facet", "grp", None, None, None),
        P(None, None, "facet", "grp"),
    )
    return jax.shard_map(
        per_device, mesh=mesh, in_specs=in_specs, out_specs=out_specs, check_vma=False
    )
```

```python
import jax
import jax.numpy as jnp
from jax import lax
from jax.experimental import pallas as pl
from jax.experimental.pallas import tpu as pltpu
from jax.sharding import PartitionSpec as P

ITERS = 2
NB = 8
C = 16
R = 16
L = 128
W = 3
TAPS = 7
RB = 8
KDEV = 16
NT3 = 24
VB = 256
RE = R + 2 * W
BAND = 3 * R
F32 = jnp.float32
BF16 = jnp.bfloat16

VMEM = pl.BlockSpec(memory_space=pltpu.VMEM)


def lanes():
    return lax.broadcasted_iota(jnp.int32, (C, L), 1)


def roll(x, shift):
    shift = shift % L
    return x if shift == 0 else pltpu.roll(x, shift, 1)


def is_odd(axis):
    return lax.rem(lax.axis_index(axis), 2) == 1


def pack(rows):
    total = rows[0]
    for i in range(1, len(rows)):
        total = total + roll(rows[i], 8 * i)
    return total


def unpack(packed, i, lane):
    return jnp.where(lane < 6, roll(packed, -8 * i), 0.0)


def swap_blocks(xs):
    xs = list(xs)
    lane = lanes()
    for bit in range(3):
        m = 1 << bit
        low = (lane // (16 * m)) % 2 == 0
        for i in range(8):
            if i & m == 0:
                a, b = xs[i], xs[i | m]
                xs[i] = jnp.where(low, a, roll(b, 16 * m))
                xs[i | m] = jnp.where(low, roll(a, -16 * m), b)
    return xs


def build_columns(col_taps, high, low):
    strip = 8
    for start in range(0, L, strip):
        j = start + lax.broadcasted_iota(jnp.int32, (strip, L), 0)
        n = lax.broadcasted_iota(jnp.int32, (strip, L), 1)
        outside = jnp.where(n < W, n - W, jnp.where(n < 2 * W, n - W + L, 2 * L))
        edge = start == 0 or start == L - strip
        for tile, place in ((0, n), (1, outside)):
            tap = place - j + W
            for b in range(NB):
                value = jnp.zeros((strip, L), F32)
                if tile == 0 or edge:
                    for e in range(TAPS):
                        value = jnp.where(tap == e, col_taps[e, b], value)
                rounded = value.astype(BF16)
                rows, cols = slice(b * L + start, b * L + start + strip), slice(tile * L, (tile + 1) * L)
                high[rows, cols] = rounded
                low[rows, cols] = (value - rounded.astype(F32)).astype(BF16)


def times(tap, row):
    return (tap[None] * row.reshape(2, C // 2, L)).reshape(C, L)


def filter_row(row_taps, b, terms):
    total = None
    for a, row in terms:
        term = times(row_taps[a, b], row)
        total = term if total is None else total + term
    return total


def back_project(vb, blocks, across, row_ids, col_ids, contrib, sums):
    sums[...] = jnp.zeros(sums.shape, F32)
    for k in range(KDEV):
        contrib[k] = lax.dot_general(
            vb[row_ids[k]], blocks[k], (((1,), (int(across),)), ((), ())), preferred_element_type=F32
        )
    for k in range(KDEV):
        q = col_ids[k]
        sums[q] = sums[q] + contrib[k]


def turn_kernel(blocks, after, turned):
    for k in range(KDEV):
        turned[k] = blocks[k].T


def synth_rows(row_taps, b, rows, places, wide_h, wide_l):
    for spot, i in enumerate(places):
        terms = [(a, rows[i - a]) for a in range(TAPS) if 0 <= i - a < R]
        total = filter_row(row_taps, b, terms)
        high = total.astype(BF16)
        wide_h[spot * C : (spot + 1) * C, b * L : (b + 1) * L] = high
        if wide_l is not None:
            low = (total - high.astype(F32)).astype(BF16)
            wide_l[spot * C : (spot + 1) * C, b * L : (b + 1) * L] = low


OUTER = tuple(range(W)) + tuple(range(R + W, RE))


def filter_columns(rows_h, rows_l, col_h, col_l):
    return (
        jnp.dot(rows_h, col_h[...], preferred_element_type=F32)
        + jnp.dot(rows_l, col_h[...], preferred_element_type=F32)
        + jnp.dot(rows_h, col_l[...], preferred_element_type=F32)
    )


def make_message(sums, wide_h, wide_l, col_h, col_l, smooth, msg):
    odd = is_odd("facet")
    tile_row = jnp.where(odd, 0, 2)
    top = pl.multiple_of(jnp.where(odd, 0, W * C), C)
    smooth[...] = filter_columns(
        wide_h[pl.ds(top, W * C), :], wide_l[pl.ds(top, W * C), :], col_h, col_l
    )
    for h in range(2):
        xs = swap_blocks([sums[tile_row * 8 + t, :, h * L : (h + 1) * L] for t in range(8)])
        for i in range(8):
            r = h * 8 + i
            value = xs[i]
            if r < W:
                value = value + jnp.where(odd, 0.0, smooth[r * C : (r + 1) * C, :L])
            if r >= R - W:
                t = r - (R - W)
                value = value + jnp.where(odd, smooth[t * C : (t + 1) * C, :L], 0.0)
            msg[r] = value.astype(BF16)
    msg[R] = pack([smooth[i * C : (i + 1) * C, L:] for i in range(W)]).astype(BF16)


def sums_kernel(sums, u_rows, row_taps, col_h, col_l, main, ext, smooth, wide):
    for b in range(NB):
        rows = [u_rows[b, r * C : (r + 1) * C, :].astype(F32) for r in range(R)]
        synth_rows(row_taps, b, rows, range(RE), wide, None)
    smooth[...] = jnp.dot(wide[...], col_h[...], preferred_element_type=F32) + jnp.dot(
        wide[...], col_l[...], preferred_element_type=F32
    )
    for tr in range(3):
        for h in range(2):
            xs = swap_blocks([sums[tr * 8 + t, :, h * L : (h + 1) * L] for t in range(8)])
            for i in range(8):
                r = tr * R + h * 8 + i
                t = r - (R - W)
                value = xs[i]
                if 0 <= t < RE:
                    value = value + smooth[t * C : (t + 1) * C, :L]
                main[r] = value
    for t in range(RE):
        ext[t] = smooth[t * C : (t + 1) * C, L:]


def fetch(sources, targets, sems):
    copies = [pltpu.make_async_copy(s, t, sems.at[i]) for i, (s, t) in enumerate(zip(sources, targets))]
    for copy in copies:
        copy.start()
    return copies


def first_kernel(
    taps_hbm, rows_hbm, cols_hbm, u_hbm, v_hbm, blocks_hbm,
    sums, msg, u_rows, col_h, col_l, blocks, row_taps,
    row_ids, col_ids, taps, col_taps, u, v, vb, contrib, turned, smooth, wide_h, wide_l, sems,
):
    get_u, get_taps, get_v, get_blocks, get_rows, get_cols = fetch(
        (u_hbm, taps_hbm, v_hbm, blocks_hbm, rows_hbm, cols_hbm),
        (u, taps, v, blocks, row_ids, col_ids),
        sems,
    )
    get_taps.wait()
    for a in range(TAPS):
        for b in range(NB):
            row_taps[a, b] = jnp.broadcast_to(taps[a, 0:1, b : b + 1], (C // 2, L))
            col_taps[a, b] = jnp.broadcast_to(taps[a, 1:2, b : b + 1], (C // 2, L))
    get_u.wait()
    for b in range(NB):
        turned[b] = u[b].astype(F32)
    build_columns(col_taps, col_h, col_l)

    def wavelets(b):
        rows = [turned[b, pl.ds(r, C, stride=R), :] for r in range(R)]
        for r in range(R):
            u_rows[b, r * C : (r + 1) * C, :] = rows[r].astype(BF16)
        synth_rows(row_taps, b, rows, OUTER, wide_h, wide_l)

    for b in range(NB):
        wavelets(b)
    get_v.wait()
    get_rows.wait()
    get_cols.wait()
    get_blocks.wait()
    vb[...] = v[...].astype(BF16)
    back_project(vb, blocks, True, row_ids, col_ids, contrib, sums)
    make_message(sums, wide_h, wide_l, col_h, col_l, smooth, msg)


def pair_kernel(with_image, *refs):
    if with_image:
        main, ext, got, image, total, total_ext, msg = refs
    else:
        main, ext, got, total, total_ext, msg = refs
    odd = is_odd("facet")
    lane = lanes()
    for r in range(R):
        row = main[R + r] + got[r].astype(F32)
        total[r] = row
        msg[R + r] = row.astype(BF16)
        total_ext[r] = ext[W + r]
    spot = jnp.where(odd, 0, R - W)
    packed = got[R].astype(F32)
    for i in range(W):
        total_ext[spot + i] = total_ext[spot + i] + unpack(packed, i, lane)
    far = jnp.where(odd, 2 * R, 0)
    far_ext = jnp.where(odd, R + W, 0)
    for r in range(R):
        msg[r] = main[far + r].astype(BF16)
    msg[2 * R] = pack([total_ext[r] for r in range(R)]).astype(BF16)
    msg[2 * R + 1] = pack([ext[far_ext + i] for i in range(W)]).astype(BF16)
    if with_image:
        for r in range(R):
            msg[2 * R + 2 + r] = image[pl.ds(r, C, stride=R), :].astype(BF16)


def rim_kernel(with_image, *refs):
    if with_image:
        total, total_ext, main, ext, got, image, _, part, part_ext, msg_a, msg_b, x = refs
    else:
        total, total_ext, main, ext, got, part, part_ext, msg_a, msg_b = refs
    odd = is_odd("facet")
    lane = lanes()
    far = jnp.where(odd, 2 * R, 0)
    far_ext = jnp.where(odd, R + W, 0)
    packed = got[2 * R].astype(F32)
    for r in range(R):
        part[r] = total[r] + got[r].astype(F32)
        part_ext[r] = total_ext[r]
        part[R + r] = got[R + r].astype(F32) + main[far + r]
        part_ext[R + r] = unpack(packed, r, lane)
    near = jnp.where(odd, R - W, 0)
    away = jnp.where(odd, 0, R - W)
    packed = got[2 * R + 1].astype(F32)
    for i in range(W):
        part_ext[near + i] = part_ext[near + i] + unpack(packed, i, lane)
        part_ext[R + away + i] = part_ext[R + away + i] + ext[far_ext + i]
    if with_image:
        for r in range(R):
            x[r] = image[pl.ds(r, C, stride=R), :]
            x[R + r] = got[2 * R + 2 + r].astype(F32)
    godd = is_odd("grp")
    slot = lane // 8
    sub = lane % 8
    first = sub < W
    second = (sub >= W) & (sub < 2 * W)
    for p in range(2):
        left = jnp.zeros((C, L), F32)
        right = jnp.zeros((C, L), F32)
        for r in range(R):
            row, row_ext = part[p * R + r], part_ext[p * R + r]
            one = (slot == r) & first
            two = (slot == r) & second
            left = jnp.where(one, roll(row_ext, 8 * r), left)
            left = jnp.where(two, roll(row, 8 * r + W), left)
            right = jnp.where(one, roll(row_ext, 8 * r - W), right)
            right = jnp.where(two, roll(row, 8 * r + 2 * W), right)
        msg_a[p] = jnp.where(godd, left, right).astype(BF16)
        msg_b[p] = jnp.where(godd, right, left).astype(BF16)
        if with_image:
            left = jnp.zeros((C, L), F32)
            right = jnp.zeros((C, L), F32)
            for r in range(R):
                row = x[p * R + r]
                one = (slot == r) & first
                left = jnp.where(one, roll(row, 8 * r), left)
                right = jnp.where(one, roll(row, 8 * r + W), right)
            msg_a[2 + p] = jnp.where(godd, left, right).astype(BF16)
            msg_b[2 + p] = jnp.where(godd, right, left).astype(BF16)


def primal_kernel(first, last, *refs):
    refs = list(refs)
    part, part_ext, got_a, got_b, x = refs[:5]
    refs = refs[5:]
    if not first:
        x_ext = refs.pop(0)
    if last:
        image_out, e, e_ext, msg, turned = refs
    else:
        new_x, new_x_ext, e, e_ext, msg = refs
    lane = lanes()
    facet, grp = lax.axis_index("facet"), lax.axis_index("grp")
    odd = is_odd("facet")
    godd = is_odd("grp")
    on_left = (grp > 0) & (lane < W)
    on_right = (grp < lax.axis_size("grp") - 1) & (lane >= W) & (lane < 2 * W)
    inside = on_left | on_right
    there = jnp.where(odd, facet < lax.axis_size("facet") - 1, facet > 0)
    got_a_wide = got_a[...].astype(F32)
    got_b_wide = got_b[...].astype(F32)
    from_left = jnp.where(godd, got_a_wide, got_b_wide)
    from_right = jnp.where(godd, got_b_wide, got_a_wide)
    rims = []
    for p in range(2):
        for r in range(R):
            i = p * R + r
            grad = part[i] + jnp.where(lane < W, roll(from_left[p], -8 * r), 0.0)
            grad = grad + jnp.where(lane >= L - W, roll(from_right[p], -8 * r - W), 0.0)
            rim = jnp.where(
                lane < W, roll(from_left[p], -8 * r - W), roll(from_right[p], -8 * r)
            )
            grad_ext = part_ext[i] + rim
            old = x[i]
            if first:
                old_ext = jnp.where(
                    lane < W, roll(from_left[2 + p], -8 * r), roll(from_right[2 + p], -8 * r + W)
                )
            else:
                old_ext = x_ext[i]
            new = jnp.maximum(old - 0.5 * grad, 0.0)
            new_ext = jnp.maximum(old_ext - 0.5 * grad_ext, 0.0)
            ahead = 2.0 * new - old
            ahead_ext = jnp.where(inside, 2.0 * new_ext - old_ext, 0.0)
            if p == 1:
                ahead = jnp.where(there, ahead, 0.0)
                ahead_ext = jnp.where(there, ahead_ext, 0.0)
            e[i] = ahead.astype(BF16)
            e_ext[i] = ahead_ext.astype(BF16)
            if p == 0:
                msg[r] = ahead.astype(BF16)
                rims.append(ahead_ext)
                if last:
                    turned[r * C : (r + 1) * C, :] = new
            if not last:
                new_x[i] = new
                new_x_ext[i] = new_ext
    msg[R] = pack(rims).astype(BF16)
    if last:
        for c in range(C):
            image_out[c * R : (c + 1) * R, :] = turned[pl.ds(c, R, stride=C), :]


def shrunk(u_row, coefficient, limit):
    full = u_row.astype(F32) + 0.5 * coefficient
    size = jnp.sqrt(jnp.sum(full * full, axis=0, keepdims=True))
    return full * (limit / jnp.maximum(size, limit))


def near_kernel(e, e_ext, col_h, col_l, row_taps, u_rows, thr, flat, wide, edge, middle):
    odd = is_odd("facet")
    base_b = jnp.where(odd, 2, 0)
    for tile_row, base in ((1, 0), (base_b, R)):
        for h in range(2):
            xs = swap_blocks([e[base + h * 8 + i].astype(F32) for i in range(8)])
            for t in range(8):
                flat[tile_row * 8 + t, :, h * L : (h + 1) * L] = xs[t].astype(BF16)
    near = jnp.concatenate([e[:R].reshape(R * C, L), e_ext[:R].reshape(R * C, L)], axis=1)
    wide[...] = spread_columns(near, col_h, col_l)
    start = jnp.where(odd, R, 2 * R - W)
    for i in range(W):
        edge[i * C : (i + 1) * C, :L] = e[start + i]
        edge[i * C : (i + 1) * C, L:] = e_ext[start + i]
    for b in range(NB):
        cols = slice(b * L, (b + 1) * L)
        for r in range(W, R - W):
            terms = [(a, wide[(r - W + a) * C : (r - W + a + 1) * C, cols]) for a in range(TAPS)]
            new = shrunk(
                u_rows[b, r * C : (r + 1) * C, :], filter_row(row_taps, b, terms), thr[b, r : r + 1, :]
            )
            middle[b, (r - W) * C : (r - W + 1) * C, :] = new.astype(BF16)


def spread_columns(rows, col_h, col_l):
    both = (((1,), (1,)), ((), ()))
    return lax.dot_general(rows, col_h[...], both, preferred_element_type=F32) + lax.dot_general(
        rows, col_l[...], both, preferred_element_type=F32
    )


def dual_kernel(last, *refs):
    flat_in, inner, edge, middle, got, v, vis, blocks, u_rows, thr, col_h, col_l = refs[:12]
    row_taps, radii, rows_vmem, cols_vmem = refs[12:16]
    refs = refs[16:]
    if last:
        image, image_hbm, v_hbm, u_hbm, *refs = refs
        v_out, u_out, turned, out_sems, *refs = refs
    else:
        blocks_turned, sums, msg, v_out, u_out, *refs = refs
        vb, tiles, smooth, wide_h, wide_l, *refs = refs
    row_ids, col_ids, sems, flat, wide, edges, contrib, totals = refs
    get_rows, get_cols = fetch((rows_vmem, cols_vmem), (row_ids, col_ids), sems)
    puts = []
    if last:
        put = pltpu.make_async_copy(image, image_hbm, out_sems.at[NB + 1])
        put.start()
        puts.append(put)
    odd = is_odd("facet")
    lane = lanes()
    packed = got[R].astype(F32)
    near_a = jnp.where(odd, R - W, 0)
    above, below = edges.at[0], edges.at[1]
    for i in range(W):
        rows = slice(i * C, (i + 1) * C)
        mine = edge[rows, :]
        rim = jnp.where(odd, roll(packed, -8 * (R - W + i)), roll(packed, -8 * i))
        theirs = jnp.concatenate(
            [got[near_a + i], jnp.where(lane < 2 * W, rim, 0.0).astype(BF16)], axis=1
        )
        above[rows, :] = jnp.where(odd, theirs, mine)
        below[rows, :] = jnp.where(odd, mine, theirs)
    wide[: W * C, :] = spread_columns(above[...], col_h, col_l)
    wide[W * C :, :] = spread_columns(below[...], col_h, col_l)
    tile_a = jnp.where(odd, 0, 2)
    tile_b = jnp.where(odd, 2, 0)
    for h in range(2):
        xs = swap_blocks([got[h * 8 + i].astype(F32) for i in range(8)])
        for t in range(8):
            flat[tile_a * 8 + t, :, h * L : (h + 1) * L] = xs[t].astype(BF16)
    for t in range(8):
        flat[8 + t] = flat_in[8 + t]
        flat[tile_b * 8 + t] = flat_in[tile_b * 8 + t]

    def operators():
        totals[...] = jnp.zeros(totals.shape, F32)
        for k in range(KDEV):
            contrib[k] = jnp.dot(flat[col_ids[k]], blocks[k], preferred_element_type=F32)
        for k in range(KDEV):
            r = row_ids[k]
            totals[r] = totals[r] + contrib[k]
        for r in range(RB):
            seen = vis[r]
            moved = v[r] + 0.5 * totals[r]
            offset = 2.0 * moved - seen
            length = jnp.sqrt(
                jnp.sum(jnp.sum(offset * offset, axis=1, keepdims=True), axis=0, keepdims=True)
            )
            radius = radii[0:1, r : r + 1]
            scale = radius / jnp.maximum(length, radius)
            new = moved - 0.5 * (seen + offset * scale)
            v_out[r] = new
            if not last:
                vb[r] = new.astype(BF16)
        if last:
            put = pltpu.make_async_copy(v_out, v_hbm, out_sems.at[NB])
            put.start()
            puts.append(put)
        else:
            back_project(vb, blocks_turned, False, row_ids, col_ids, tiles, sums)

    def filtered(t, b):
        cols = slice(b * L, (b + 1) * L)
        if t < W:
            return wide[t * C : (t + 1) * C, cols]
        if t < W + R:
            return inner[(t - W) * C : (t - W + 1) * C, cols]
        return wide[(t - R) * C : (t - R + 1) * C, cols]

    def wavelets(bases):
        for b in bases:
            rows = []
            for r in range(R):
                if W <= r < R - W:
                    new = middle[b, (r - W) * C : (r - W + 1) * C, :]
                else:
                    new = shrunk(
                        u_rows[b, r * C : (r + 1) * C, :],
                        filter_row(row_taps, b, [(a, filtered(r + a, b)) for a in range(TAPS)]),
                        thr[b, r : r + 1, :],
                    ).astype(BF16)
                if last:
                    turned[b, r * C : (r + 1) * C, :] = new.astype(F32)
                else:
                    u_out[b, r * C : (r + 1) * C, :] = new
                    rows.append(new.astype(F32))
            if last:
                for c in range(C):
                    u_out[b, c * R : (c + 1) * R, :] = turned[b, pl.ds(c, R, stride=C), :].astype(BF16)
                put = pltpu.make_async_copy(u_out.at[b], u_hbm.at[b], out_sems.at[b])
                put.start()
                puts.append(put)
            else:
                synth_rows(row_taps, b, rows, OUTER, wide_h, wide_l)

    wavelets(range(NB))
    get_rows.wait()
    get_cols.wait()
    operators()
    for put in puts:
        put.wait()
    if not last:
        make_message(sums, wide_h, wide_l, col_h, col_l, smooth, msg)


def shape(dims, dtype=F32):
    return jax.ShapeDtypeStruct(dims, dtype)


def scratch(*dims, dtype=F32):
    return pltpu.VMEM(dims, dtype)


def small(dims, dtype):
    return pltpu.SMEM(dims, dtype)


HALF = [shape((NT3, C, VB)), shape((R + 1, C, L), BF16)]
OUTER_TEMPS = [
    scratch(2 * W * C, NB * L, dtype=BF16),
    scratch(2 * W * C, NB * L, dtype=BF16),
]


def call(kernel, far, arrays, outs, temps=(), name=None, mib=8, final=0):
    far = [pltpu.with_memory_space_constraint(a, pltpu.HBM) for a in far]
    arrays = [pltpu.with_memory_space_constraint(a, pltpu.VMEM) for a in arrays]
    anywhere = pl.BlockSpec(memory_space=pl.ANY)
    return pl.pallas_call(
        kernel,
        out_shape=tuple(
            (pltpu.HBM if i < final else pltpu.VMEM)(o.shape, o.dtype) for i, o in enumerate(outs)
        ),
        in_specs=[anywhere] * len(far) + [VMEM] * len(arrays),
        out_specs=tuple(anywhere if i < final else VMEM for i in range(len(outs))),
        scratch_shapes=list(temps),
        compiler_params=pltpu.CompilerParams(vmem_limit_bytes=mib << 20),
        name=name,
    )(*far, *arrays)


def pairs_of(axis):
    count = lax.axis_size(axis)
    inner = [(i, i ^ 1) for i in range(count)]
    outer = [(i, ((i + 1) ^ 1) - 1) for i in range(1, count - 1)]
    return inner, outer


def per_device(
    image, wavelet_dual, thresholds, filter_taps, visibilities,
    data_dual, ball_radii, blocks, row_index, col_index,
):
    image_rows = image.reshape(C * R, L)
    u = wavelet_dual.reshape(NB, C * R, L)
    seen, v = visibilities[0, 0], data_dual[0, 0]
    radii, row_ids, col_ids = ball_radii[0], row_index[0, 0], col_index[0, 0]
    taps = filter_taps.transpose(2, 1, 0)
    facet_in, facet_out = pairs_of("facet")
    grp_in, grp_out = pairs_of("grp")
    scalars = [small((KDEV,), jnp.int32), small((KDEV,), jnp.int32)]
    sums, msg, u, col_h, col_l, operators, row_taps = call(
        first_kernel,
        (taps, row_ids, col_ids, u, v, blocks[0, 0]),
        (),
        HALF
        + [
            shape((NB, R * C, L), BF16),
            shape((NB * L, 2 * L), BF16),
            shape((NB * L, 2 * L), BF16),
            shape((KDEV, VB, VB), BF16),
            shape((TAPS, NB, C // 2, L)),
        ],
        scalars
        + [
            scratch(TAPS, 2, NB),
            scratch(TAPS, NB, C // 2, L),
            scratch(NB, C * R, L, dtype=BF16),
            scratch(RB, C, VB),
            scratch(RB, C, VB, dtype=BF16),
            scratch(KDEV, C, VB),
            scratch(NB, C * R, L),
            scratch(W * C, 2 * L),
            *OUTER_TEMPS,
            pltpu.SemaphoreType.DMA((6,)),
        ],
        name="first",
        mib=16,
    )
    x = x_ext = None
    for iteration in range(ITERS):
        first, last = iteration == 0, iteration == ITERS - 1
        got = lax.ppermute(msg, "facet", facet_in)
        main, ext = call(
            sums_kernel,
            (),
            (sums, u, row_taps, col_h, col_l),
            [shape((BAND, C, L)), shape((RE, C, L))],
            [
                scratch(RE * C, 2 * L),
                scratch(RE * C, NB * L, dtype=BF16),
            ],
            name="sums",
        )
        total, total_ext, msg = call(
            lambda *refs: pair_kernel(first, *refs),
            (),
            (main, ext, got) + ((image_rows,) if first else ()),
            [
                shape((R, C, L)),
                shape((R, C, L)),
                shape(((3 if first else 2) * R + 2, C, L), BF16),
            ],
            name="pair",
        )
        got = lax.ppermute(msg, "facet", facet_out)
        if first:
            (turned,) = call(
                turn_kernel, (), (operators, total), [shape((KDEV, VB, VB), BF16)], name="turn", mib=4
            )
        rim = shape((4 if first else 2, C, L), BF16)
        part, part_ext, msg_a, msg_b, *rest = call(
            lambda *refs: rim_kernel(first, *refs),
            (),
            (total, total_ext, main, ext, got) + ((image_rows, turned) if first else ()),
            [shape((2 * R, C, L)), shape((2 * R, C, L)), rim, rim]
            + ([shape((2 * R, C, L))] if first else []),
            name="rim",
        )
        if first:
            x = rest[0]
        got_a = lax.ppermute(msg_a, "grp", grp_in)
        got_b = lax.ppermute(msg_b, "grp", grp_out)
        wide = shape((2 * R, C, L))
        outs = [shape((2 * R, C, L), BF16), shape((2 * R, C, L), BF16), shape((R + 1, C, L), BF16)]
        results = call(
            lambda *refs: primal_kernel(first, last, *refs),
            (),
            (part, part_ext, got_a, got_b, x) + (() if first else (x_ext,)),
            ([shape((C * R, L))] if last else [wide, wide]) + outs,
            [scratch(R * C, L)] if last else [],
            name="primal",
        )
        e, e_ext, msg = results[-3:]
        if last:
            image_out = results[0]
        else:
            x, x_ext = results[:2]
        got = lax.ppermute(msg, "facet", facet_in)
        flat, inner, edge, middle = call(
            near_kernel,
            (),
            (e, e_ext, col_h, col_l, row_taps, u, thresholds),
            [
                shape((NT3, C, VB), BF16),
                shape((R * C, NB * L)),
                shape((W * C, 2 * L), BF16),
                shape((NB, (R - 2 * W) * C, L), BF16),
            ],
            name="near",
        )
        outs = [shape((RB, C, VB)), shape((NB, R * C, L), BF16)]
        if last:
            outs = [shape((C * R, L))] + outs
            temps = [
                scratch(RB, C, VB),
                scratch(NB, C * R, L, dtype=BF16),
                scratch(NB, R * C, L),
                pltpu.SemaphoreType.DMA((NB + 2,)),
            ]
        else:
            temps = [
                scratch(RB, C, VB, dtype=BF16),
                scratch(KDEV, C, VB),
                scratch(W * C, 2 * L),
                *OUTER_TEMPS,
            ]
        *half, v, u = call(
            lambda *refs: dual_kernel(last, *refs),
            (),
            (flat, inner, edge, middle, got, v, seen, operators, u, thresholds, col_h, col_l)
            + (row_taps, radii, row_ids, col_ids)
            + ((image_out,) if last else (turned,)),
            ([] if last else HALF) + outs,
            temps
            + scalars
            + [
                pltpu.SemaphoreType.DMA((2,)),
                scratch(NT3, C, VB, dtype=BF16),
                scratch(2 * W * C, NB * L),
                scratch(2, W * C, 2 * L, dtype=BF16),
                scratch(KDEV, C, VB),
                scratch(RB, C, VB),
            ],
            name="dual",
            mib=16,
            final=3 if last else 0,
        )
        if last:
            (image_out,) = half
        else:
            sums, msg = half
    return (image_out.reshape(C, R, L), v[None, None], u.reshape(NB, C, R, L))


def solution(mesh):
    in_specs = (
        P(None, "facet", "grp"),
        P(None, None, "facet", "grp"),
        P(None, "facet", "grp"),
        P(),
        P("facet", "grp", None, None, None),
        P("facet", "grp", None, None, None),
        P("facet", "grp", None),
        P("facet", "grp", None, None, None),
        P("facet", "grp", None),
        P("facet", "grp", None),
    )
    out_specs = (
        P(None, "facet", "grp"),
        P("facet", "grp", None, None, None),
        P(None, None, "facet", "grp"),
    )
    return jax.shard_map(
        per_device, mesh=mesh, in_specs=in_specs, out_specs=out_specs, check_vma=False
    )
```
